512 devices in a mesh: gx: 16 (over z, core), gy: 32 (over x, y).
Axes of the slice: x: 4, y: 8, z: 8, core: 2. Of those that a mesh axis runs over, the one named last changes fastest.
Arguments:
- field: float32 [1024, 12288], P('gx', 'gy'), may hold values from -9 to 9
- decay_x: float32 [1024, 8], P('gx'), may hold values from 0.15 to 0.99999
- decay_y: float32 [1536, 8], P('gy'), may hold values from 0.15 to 0.99999
Outputs:
- smoothed: float32 [1024, 12288], P('gx', 'gy')
The draws below stay inside these ranges and needn't reach their ends.
All inputs are finite; a program needn't handle non-finite values.
Results may differ from the reference program's by a relative error of at most 0.0003.
Values sent between devices are 32-bit elements; how exact they have to be, the bound alone decides.
No kernel may reach another device: no remote copies, remote signals or barrier semaphores. Data moves between devices by JAX's collectives and lax.ppermute only.
A program may use at most 64 MiB of HBM per device.

```python
import math
import jax
import jax.numpy as jnp
from jax import lax

CX = 64
CY = 48
VERTICAL_LAYERS = 8
PASSES = 1
NX = 1024
NY = 1536


def decay_draw(key, length_scale, block):
    keys = jax.random.split(key, 4)
    lowest = 20.0
    highest = 4.0 * length_scale
    spreads = jax.random.uniform(keys[0], (VERTICAL_LAYERS,), jnp.float32)
    scale_values = lowest * (highest / lowest) ** spreads
    rough_noise = jnp.exp(jax.random.uniform(keys[1], (length_scale, VERTICAL_LAYERS), jnp.float32, math.log(0.6), math.log(1.5)))
    processor_multiplier = jnp.exp(jax.random.uniform(keys[2], (length_scale // block, VERTICAL_LAYERS), jnp.float32, math.log(0.7), math.log(1.4)))
    processor_multiplier = jnp.repeat(processor_multiplier, block, axis=0)
    probe_points = jax.random.randint(keys[3], (3, VERTICAL_LAYERS), 0, length_scale)
    grid_location = jnp.arange(length_scale)
    impulse_spike = jnp.ones((length_scale, VERTICAL_LAYERS), jnp.float32)
    for selected_index in range(3):
        impulse_spike = impulse_spike * jnp.where(grid_location[:, None] == probe_points[selected_index][None, :], 0.6, 1.0)
    decay_factors = jnp.exp(-1.0 / (scale_values[None, :] * rough_noise * processor_multiplier)) * impulse_spike
    return decay_factors.astype(jnp.float32)


def draw_decay_x(key, part):
    return decay_draw(jax.random.fold_in(key, 21), NX, CX)


def draw_decay_y(key, part):
    return decay_draw(jax.random.fold_in(key, 22), NY, CY)


def draw_field(key, part):
    keys = jax.random.split(jax.random.fold_in(key, 11), 5)
    noise = jax.random.truncated_normal(keys[0], -5.0, 5.0, (NX, NY, VERTICAL_LAYERS), jnp.float32)
    across = jnp.arange(NX, dtype=jnp.float32) / NX
    along = jnp.arange(NY, dtype=jnp.float32) / NY
    waves_x = jax.random.randint(keys[1], (3, VERTICAL_LAYERS), 1, 5).astype(jnp.float32)
    waves_y = jax.random.randint(keys[2], (3, VERTICAL_LAYERS), 1, 5).astype(jnp.float32)
    phases = jax.random.uniform(keys[3], (2, 3, VERTICAL_LAYERS), jnp.float32)
    amplitude = jax.random.uniform(keys[4], (3, VERTICAL_LAYERS), jnp.float32, -1.0, 1.0)
    smooth = jnp.zeros((NX, NY, VERTICAL_LAYERS), jnp.float32)
    for selected_index in range(3):
        first = jnp.cos(2.0 * math.pi * (waves_x[selected_index][None, :] * across[:, None] + phases[0, selected_index][None, :]))
        second = jnp.cos(2.0 * math.pi * (waves_y[selected_index][None, :] * along[:, None] + phases[1, selected_index][None, :]))
        smooth = smooth + amplitude[selected_index][None, None, :] * first[:, None, :] * second[None, :, :]
    return (noise + smooth).reshape(NX, NY * VERTICAL_LAYERS).astype(jnp.float32)


def setup_inputs(seed: int = 0) -> dict:
    arg_keys = jax.random.split(jax.random.key(seed), 4)
    field = draw_field(jax.random.fold_in(arg_keys[3], 71), 0)
    decay_x = draw_decay_x(jax.random.fold_in(arg_keys[3], 71), 0)
    decay_y = draw_decay_y(jax.random.fold_in(arg_keys[3], 71), 0)
    return dict(field=field, decay_x=decay_x, decay_y=decay_y)


def sweep(grid, decay_factors, backward):
    gains = 1.0 - decay_factors
    width = grid.shape[1]

    def advance(states, inputs):
        values, decay, gain = inputs
        first = decay * states[0] + gain * values
        second = decay * states[1] + gain * first
        third = decay * states[2] + gain * second
        fourth = decay * states[3] + gain * third
        return (first, second, third, fourth), fourth

    zero = jnp.zeros((width, VERTICAL_LAYERS), jnp.float32)
    final, outputs = lax.scan(advance, (zero, zero, zero, zero), (grid, decay_factors, gains), reverse=backward)
    return outputs


def reference(field, decay_x, decay_y):
    grid = field.reshape(NX, NY, VERTICAL_LAYERS)
    for repeat in range(PASSES):
        grid = sweep(grid, decay_x, False)
        grid = sweep(grid, decay_x, True)
        turned = jnp.transpose(grid, (1, 0, 2))
        turned = sweep(turned, decay_y, False)
        turned = sweep(turned, decay_y, True)
        grid = jnp.transpose(turned, (1, 0, 2))
    return grid.reshape(NX, NY * VERTICAL_LAYERS)
```

```python
import jax
import jax.numpy as jnp
from jax import lax
from jax.experimental import pallas as pl
from jax.experimental.pallas import tpu as pltpu
from jax.sharding import PartitionSpec as P

F32 = jnp.float32
LANES = 128
VMEM = pltpu.MemorySpace.VMEM


def iota(shape, dim):
    return lax.broadcasted_iota(jnp.int32, shape, dim)


def take_lanes(values, lanes):
    return jnp.take_along_axis(values, jnp.broadcast_to(lanes, values.shape), axis=1)


def cascade(states, value, decay, gain):
    moved = []
    for state in states:
        value = decay * state + gain * value
        moved.append(value)
    return moved


def toeplitz(column, states):
    return [
        sum((column[row - k] * states[k] for k in range(1, row + 1)), column[row] * states[0])
        for row in range(4)
    ]


def sweep(steps, states, load, decay, gain, store, reverse):
    for step in reversed(range(steps)) if reverse else range(steps):
        states = cascade(states, load(step), decay(step), gain(step))
        if store is not None:
            store(step, states[3])
    return states


def x_ends(field_ref, decay_ref, sent_ref, grid_ref, a_ref, wide_ref, out_ref):
    steps, levels = decay_ref.shape
    a_ref[:, :levels] = decay_ref[...]
    periodic = take_lanes(a_ref[...], iota((steps, LANES), 1) % levels)
    a_ref[...] = periodic
    tiles = field_ref.shape[1] // LANES
    for tile in range(tiles):
        grid_ref[:, tile, :] = field_ref[:, tile * LANES : (tile + 1) * LANES]
    grid_ref[:, tiles, :] = jnp.zeros((steps, LANES), F32)
    row, group = (iota((4, LANES), 0), iota((4, LANES), 1) // levels)
    unit = [((row == tiles) & (group == k)).astype(F32) for k in range(8)]
    load_a = lambda i: a_ref[pl.ds(i, 1), :]
    gain = lambda i: 1.0 - a_ref[pl.ds(i, 1), :]

    def keep(i, value):
        out_ref[i] = value

    ahead = sweep(steps, unit[:4], lambda i: grid_ref[i], load_a, gain, keep, False)
    back = sweep(steps, unit[4:], lambda i: out_ref[i], load_a, gain, None, True)
    ends = ahead + back
    for k in range(8):
        wide_ref[4 * k : 4 * k + 4, :] = ends[k]
    both = wide_ref[...]
    for device in range(sent_ref.shape[0]):
        sent_ref[device] = both


def y_decays(decay_ref, a_ref):
    steps, levels = decay_ref.shape
    padded = decay_ref[...]
    spread = jnp.broadcast_to(padded[:, None, :], (steps, levels, levels))
    own = iota(spread.shape, 1) == iota(spread.shape, 2)
    column = jnp.sum(jnp.where(own, spread, 0.0), axis=2, keepdims=True)
    a_ref[...] = jnp.broadcast_to(column, (steps, levels, LANES)).reshape(steps * levels, LANES)


def x_apply_y_ends(
    got_ref, grid_ref, ax_ref, ay_ref, sent_ref, wide_ref, maps_ref, s_ref, t_ref, z_ref, out_ref
):
    devices, steps = (16, grid_ref.shape[0])
    rows = got_ref.shape[0] // devices
    levels = 8
    mine = lax.axis_index("gx")
    found = got_ref[pl.ds(3, devices * 8, stride=4), :]
    lane = iota(found.shape, 1) % levels
    for k in range(5):
        maps_ref[k] = take_lanes(found, lane + 8 * k)

    def end(m, k):
        return got_ref[rows * m + 4 * k : rows * m + 4 * k + 4, :]

    def entry(k, m, value):
        return maps_ref[k, pl.ds(8 * m + value, 1), :]

    zero = jnp.zeros((4, LANES), F32)
    states = [zero] * 4
    for m in range(devices):
        for k in range(4):
            s_ref[m, k] = states[k]
        if m < devices - 1:
            moved = toeplitz([entry(0, m, k) for k in range(4)], states)
            states = [moved[k] + end(m, k) for k in range(4)]
    states = [zero] * 4
    for m in reversed(range(devices)):
        for k in range(4):
            t_ref[m, k] = states[k]
        if m > 0:
            moved = toeplitz([entry(4, m, 4 + k) for k in range(4)], states)
            turned = [
                sum(entry(k, m, 4 + r) * s_ref[m, k] for k in range(4)) + end(m, 4 + r)
                for r in range(4)
            ]
            states = [moved[k] + turned[k] for k in range(4)]
    load_a = lambda i: ax_ref[pl.ds(i, 1), :]
    gain = lambda i: 1.0 - ax_ref[pl.ds(i, 1), :]

    def keep(i, value):
        z_ref[i] = value

    start = [s_ref[mine, k] for k in range(4)]
    sweep(steps, start, lambda i: grid_ref[i], load_a, gain, keep, False)
    start = [t_ref[mine, k] for k in range(4)]
    sweep(steps, start, lambda i: z_ref[i], load_a, gain, keep, True)
    wide_ref[...] = jnp.zeros(wide_ref.shape, F32)
    for tile in range(3):
        wide_ref[tile * LANES : (tile + 1) * LANES, :steps] = z_ref[:, tile, :].T

    lane = iota((8, LANES), 1)
    unit = [(lane == steps + k).astype(F32) for k in range(8)]
    count = ay_ref.shape[0] // 8
    load = lambda ref: lambda i: ref[8 * i : 8 * i + 8, :]
    load_a = load(ay_ref)
    gain = lambda i: 1.0 - load_a(i)

    def keep_y(i, value):
        out_ref[8 * i : 8 * i + 8, :] = value

    ahead = sweep(count, unit[:4], load(wide_ref), load_a, gain, keep_y, False)
    back = sweep(count, unit[4:], load(out_ref), load_a, gain, None, True)
    low = lane < steps
    tiles = [jnp.where(low, ahead[k], pltpu.roll(back[k], steps, 1)) for k in range(4)]
    packed = jnp.zeros((8, LANES), F32)
    for k in range(4):
        for shift, ends in ((0, back), (8, ahead)):
            at = 16 * k + shift
            moved = pltpu.roll(ends[k], (at - steps) % LANES, 1)
            packed = jnp.where((lane >= at) & (lane < at + 8), moved, packed)
    tiles.append(packed)
    for device in range(sent_ref.shape[0]):
        for k in range(5):
            sent_ref[device, k] = tiles[k]


def y_apply(got_ref, wide_ref, ay_ref, field_ref, s_ref, t_ref, z_ref):
    devices = got_ref.shape[0]
    mine = lax.axis_index("gy")
    half = LANES // 2

    def entry(packed, at):
        return jnp.broadcast_to(packed[:, at : at + 1], (8, LANES))

    zero = jnp.zeros((8, LANES), F32)
    states = [zero] * 4
    for m in range(devices):
        for k in range(4):
            s_ref[m, k] = states[k]
        if m < devices - 1:
            packed = got_ref[m, 4]
            moved = toeplitz([entry(packed, 16 * k + 8) for k in range(4)], states)
            states = [moved[k] + got_ref[m, k] for k in range(4)]
    states = [zero] * 4
    for m in reversed(range(devices)):
        for k in range(4):
            t_ref[m, k] = states[k]
        if m > 0:
            packed = got_ref[m, 4]
            moved = toeplitz([entry(packed, 16 * k + 4) for k in range(4)], states)
            turned = [
                sum(entry(packed, 16 * r + k) * s_ref[m, k] for k in range(4))
                + pltpu.roll(got_ref[m, r], half, 1)
                for r in range(4)
            ]
            states = [moved[k] + turned[k] for k in range(4)]
    count = ay_ref.shape[0] // 8
    load = lambda ref: lambda i: ref[8 * i : 8 * i + 8, :]
    load_a = load(ay_ref)
    gain = lambda i: 1.0 - load_a(i)

    def keep(i, value):
        z_ref[8 * i : 8 * i + 8, :] = value

    start = [s_ref[mine, k] for k in range(4)]
    sweep(count, start, load(wide_ref), load_a, gain, keep, False)
    start = [t_ref[mine, k] for k in range(4)]
    sweep(count, start, load(z_ref), load_a, gain, keep, True)
    for tile in range(3):
        turned = z_ref[tile * LANES : (tile + 1) * LANES, :].T
        field_ref[:, tile * LANES : (tile + 1) * LANES] = turned[:half]


def call(kernel, outs, scratch, *args):
    whole = pl.BlockSpec(memory_space=VMEM)
    return pl.pallas_call(
        kernel,
        out_shape=[jax.ShapeDtypeStruct(shape, F32) for shape in outs],
        in_specs=[whole] * len(args),
        out_specs=[whole] * len(outs),
        scratch_shapes=[pltpu.VMEM(shape, F32) for shape in scratch],
    )(*args)


def body(field, decay_x, decay_y):
    along_x, along_y = (lax.axis_size("gx"), lax.axis_size("gy"))
    rows, columns = field.shape
    count = decay_y.shape[0]
    sent, grid, ax = call(
        x_ends,
        [(along_x, 32, LANES), (rows, 4, LANES), (rows, LANES)],
        [(32, LANES), (rows, 4, LANES)],
        field,
        decay_x,
    )
    got = lax.all_to_all(sent, "gx", 0, 0, tiled=True)
    (ay,) = call(y_decays, [(columns, LANES)], [], decay_y)
    sent, wide = call(
        x_apply_y_ends,
        [(along_y, 5, 8, LANES), (columns, LANES)],
        [
            (5, along_x * 8, LANES),
            (along_x, 4, 4, LANES),
            (along_x, 4, 4, LANES),
            (rows, 4, LANES),
            (columns, LANES),
        ],
        got.reshape(along_x * 32, LANES),
        grid,
        ax,
        ay,
    )
    got = lax.all_to_all(sent, "gy", 0, 0, tiled=True)
    (out,) = call(
        y_apply,
        [(rows, columns)],
        [(along_y, 4, 8, LANES), (along_y, 4, 8, LANES), (columns, LANES)],
        got,
        wide,
        ay,
    )
    return out


def solution(mesh):
    placed = (P("gx", "gy"), P("gx", None), P("gy", None))
    return jax.shard_map(body, mesh=mesh, in_specs=placed, out_specs=P("gx", "gy"), check_vma=False)
```

```python
import functools

import jax
import jax.numpy as jnp
from jax import lax
from jax.experimental import pallas as pl
from jax.experimental.pallas import tpu as pltpu
from jax.sharding import PartitionSpec as P

F32 = jnp.float32
LANES = 128
VMEM = pltpu.MemorySpace.VMEM


def iota(shape, dim):
    return lax.broadcasted_iota(jnp.int32, shape, dim)


def take_lanes(values, lanes):
    return jnp.take_along_axis(values, jnp.broadcast_to(lanes, values.shape), axis=1)


def cascade(states, value, decay, gain):
    moved = []
    for state in states:
        value = decay * state + gain * value
        moved.append(value)
    return moved


def toeplitz(column, states):
    return [
        sum((column[row - k] * states[k] for k in range(1, row + 1)), column[row] * states[0])
        for row in range(4)
    ]


def sweep(steps, states, load, decay, gain, store, reverse):
    for step in reversed(range(steps)) if reverse else range(steps):
        states = cascade(states, load(step), decay(step), gain(step))
        if store is not None:
            store(step, states[3])
    return states


def x_ends(field_ref, decay_ref, sent_ref, grid_ref, a_ref, wide_ref, out_ref):
    levels, steps = decay_ref.shape
    a_ref[...] = jnp.concatenate([decay_ref[...]] * (LANES // levels), axis=0).T
    tiles = field_ref.shape[1] // LANES
    for tile in range(tiles):
        grid_ref[:, tile, :] = field_ref[:, tile * LANES : (tile + 1) * LANES]
    grid_ref[:, tiles, :] = jnp.zeros((steps, LANES), F32)
    row, group = (iota((4, LANES), 0), iota((4, LANES), 1) // levels)
    unit = [((row == tiles) & (group == k)).astype(F32) for k in range(8)]
    load_a = lambda i: a_ref[pl.ds(i, 1), :]
    gain = lambda i: 1.0 - a_ref[pl.ds(i, 1), :]

    def keep(i, value):
        out_ref[i] = value

    ahead = sweep(steps, unit[:4], lambda i: grid_ref[i], load_a, gain, keep, False)
    back = sweep(steps, unit[4:], lambda i: out_ref[i], load_a, gain, None, True)
    ends = ahead + back
    for k in range(8):
        wide_ref[4 * k : 4 * k + 4, :] = ends[k]
    both = wide_ref[...]
    for device in range(sent_ref.shape[0]):
        sent_ref[device] = both


def y_decays(decay_ref, a_ref):
    decays = decay_ref[...]
    for step in range(decays.shape[1]):
        a_ref[8 * step : 8 * step + 8, :] = lane_of(decays, step)


def lane_of(values, at):
    return jnp.broadcast_to(values[:, at : at + 1], (8, LANES))


def pack(ahead, back, lane):
    half = LANES // 2
    tiles = [jnp.where(lane < half, ahead[k], pltpu.roll(back[k], half, 1)) for k in range(4)]
    packed = jnp.zeros((8, LANES), F32)
    for k in range(4):
        for shift, ends in ((0, back), (8, ahead)):
            at = 16 * k + shift
            moved = pltpu.roll(ends[k], (at - half) % LANES, 1)
            packed = jnp.where((lane >= at) & (lane < at + 8), moved, packed)
    return [*tiles, packed]


def chained(got_ref, ahead, back, s_ref, t_ref):
    blocks, half = (got_ref.shape[0], LANES // 2)
    low = iota((8, LANES), 1) < half
    for m in range(blocks):
        packed = got_ref[m, 4]
        for k in range(4):
            s_ref[m, k] = ahead[k]
        moved = toeplitz([lane_of(packed, 16 * k + 8) for k in range(4)], ahead)
        ahead = [moved[k] + jnp.where(low, got_ref[m, k], 0.0) for k in range(4)]
    for m in reversed(range(blocks)):
        packed = got_ref[m, 4]
        for k in range(4):
            t_ref[m, k] = back[k]
        moved = toeplitz([lane_of(packed, 16 * k + 4) for k in range(4)], back)
        turned = [
            sum(lane_of(packed, 16 * r + k) * s_ref[m, k] for k in range(4))
            + jnp.where(low, pltpu.roll(got_ref[m, r], half, 1), 0.0)
            for r in range(4)
        ]
        back = [moved[k] + turned[k] for k in range(4)]
    return ahead, back


def x_apply_y_ends(
    got_ref, grid_ref, ax_ref, ay_ref, sent_ref, wide_ref, maps_ref, s_ref, t_ref, z_ref, out_ref
):
    steps = grid_ref.shape[0]
    devices, rows = (s_ref.shape[0], 32)
    mine = lax.axis_index("gx")
    found = got_ref[pl.ds(3, devices * 8, stride=4), :]
    lane = iota(found.shape, 1) % 8
    for k in range(5):
        maps_ref[k] = take_lanes(found, lane + 8 * k)

    def end(m, k):
        return got_ref[rows * m + 4 * k : rows * m + 4 * k + 4, :]

    def entry(k, m, value):
        return maps_ref[k, pl.ds(8 * m + value, 1), :]

    zero = jnp.zeros((4, LANES), F32)
    states = [zero] * 4
    for m in range(devices):
        for k in range(4):
            s_ref[m, k] = states[k]
        if m < devices - 1:
            moved = toeplitz([entry(0, m, k) for k in range(4)], states)
            states = [moved[k] + end(m, k) for k in range(4)]
    states = [zero] * 4
    for m in reversed(range(devices)):
        for k in range(4):
            t_ref[m, k] = states[k]
        if m > 0:
            moved = toeplitz([entry(4, m, 4 + k) for k in range(4)], states)
            turned = [
                sum(entry(k, m, 4 + r) * s_ref[m, k] for k in range(4)) + end(m, 4 + r)
                for r in range(4)
            ]
            states = [moved[k] + turned[k] for k in range(4)]
    load_a = lambda i: ax_ref[pl.ds(i, 1), :]
    gain = lambda i: 1.0 - ax_ref[pl.ds(i, 1), :]

    def keep(i, value):
        z_ref[i] = value

    start = [s_ref[mine, k] for k in range(4)]
    sweep(steps, start, lambda i: grid_ref[i], load_a, gain, keep, False)
    start = [t_ref[mine, k] for k in range(4)]
    sweep(steps, start, lambda i: z_ref[i], load_a, gain, keep, True)
    wide_ref[...] = jnp.zeros(wide_ref.shape, F32)
    for tile in range(3):
        wide_ref[tile * LANES : (tile + 1) * LANES, :steps] = z_ref[:, tile, :].T

    lane = iota((8, LANES), 1)
    unit = [(lane == steps + k).astype(F32) for k in range(8)]
    count = ay_ref.shape[0] // 8
    load = lambda ref: lambda i: ref[8 * i : 8 * i + 8, :]
    load_a = load(ay_ref)
    gain = lambda i: 1.0 - load_a(i)

    def keep_y(i, value):
        out_ref[8 * i : 8 * i + 8, :] = value

    ahead = sweep(count, unit[:4], load(wide_ref), load_a, gain, keep_y, False)
    back = sweep(count, unit[4:], load(out_ref), load_a, gain, None, True)
    tiles = pack(ahead, back, lane)
    for device in range(sent_ref.shape[0]):
        for k in range(5):
            sent_ref[device, k] = tiles[k]


def y_join(got_ref, sent_ref, mine_ref, s_ref, t_ref):
    blocks = got_ref.shape[0]
    lane = iota((8, LANES), 1)
    unit = [(lane == LANES // 2 + k).astype(F32) for k in range(8)]
    ahead, back = chained(got_ref, unit[:4], unit[4:], s_ref, t_ref)
    tiles = pack(ahead, back, lane)
    for device in range(sent_ref.shape[0]):
        for k in range(5):
            sent_ref[device, k] = tiles[k]
    mine = lax.axis_index("gy") % blocks
    for k in range(4):
        mine_ref[k] = s_ref[mine, k]
        mine_ref[4 + k] = t_ref[mine, k]


def y_apply(got_ref, mine_ref, wide_ref, ay_ref, field_ref, s_ref, t_ref, z_ref, *, blocks):
    half = LANES // 2
    zero = [jnp.zeros((8, LANES), F32)] * 4
    chained(got_ref, zero, zero, s_ref, t_ref)
    mine = lax.axis_index("gy") // blocks
    ahead = [s_ref[mine, k] for k in range(4)]
    back = [t_ref[mine, k] for k in range(4)]

    def entered(k, starts):
        found = mine_ref[k]
        return found + sum(lane_of(found, half + at) * state for at, state in starts)

    first = [(k, ahead[k]) for k in range(4)]
    both = first + [(4 + k, back[k]) for k in range(4)]
    ahead = [entered(k, first[: k + 1]) for k in range(4)]
    back = [entered(4 + k, both[: 5 + k]) for k in range(4)]
    count = ay_ref.shape[0] // 8
    load = lambda ref: lambda i: ref[8 * i : 8 * i + 8, :]
    load_a = load(ay_ref)
    gain = lambda i: 1.0 - load_a(i)

    def keep(i, value):
        z_ref[8 * i : 8 * i + 8, :] = value

    sweep(count, ahead, load(wide_ref), load_a, gain, keep, False)
    sweep(count, back, load(z_ref), load_a, gain, keep, True)
    for tile in range(3):
        turned = z_ref[tile * LANES : (tile + 1) * LANES, :].T
        field_ref[:, tile * LANES : (tile + 1) * LANES] = turned[:half]


def call(kernel, outs, scratch, *args):
    whole = pl.BlockSpec(memory_space=VMEM)
    return pl.pallas_call(
        kernel,
        out_shape=[VMEM(shape, F32) for shape in outs],
        in_specs=[whole] * len(args),
        out_specs=[whole] * len(outs),
        scratch_shapes=[pltpu.VMEM(shape, F32) for shape in scratch],
        compiler_params=pltpu.CompilerParams(vmem_limit_bytes=16 << 20),
    )(*(pltpu.with_memory_space_constraint(a, VMEM) for a in args))


def body(field, decay_x, decay_y):
    along_x, along_y = (lax.axis_size("gx"), lax.axis_size("gy"))
    blocks = 8
    rows_y = along_y // blocks
    rows, columns = field.shape
    sent, grid, ax = call(
        x_ends,
        [(along_x, 32, LANES), (rows, 4, LANES), (rows, LANES)],
        [(32, LANES), (rows, 4, LANES)],
        field,
        decay_x.T,
    )
    got = lax.all_to_all(sent, "gx", 0, 0, tiled=True)
    (ay,) = call(y_decays, [(columns, LANES)], [], decay_y.T)
    sent, wide = call(
        x_apply_y_ends,
        [(blocks, 5, 8, LANES), (columns, LANES)],
        [
            (5, along_x * 8, LANES),
            (along_x, 4, 4, LANES),
            (along_x, 4, 4, LANES),
            (rows, 4, LANES),
            (columns, LANES),
        ],
        got.reshape(along_x * 32, LANES),
        grid,
        ax,
        ay,
    )
    near = [[blocks * r + k for k in range(blocks)] for r in range(rows_y)]
    got = lax.all_to_all(sent, "gy", 0, 0, tiled=True, axis_index_groups=near)
    sent, own = call(
        y_join,
        [(rows_y, 5, 8, LANES), (8, 8, LANES)],
        [(blocks, 4, 8, LANES), (blocks, 4, 8, LANES)],
        got,
    )
    far = [[blocks * r + k for r in range(rows_y)] for k in range(blocks)]
    got = lax.all_to_all(sent, "gy", 0, 0, tiled=True, axis_index_groups=far)
    (out,) = call(
        functools.partial(y_apply, blocks=blocks),
        [(rows, columns)],
        [(rows_y, 4, 8, LANES), (rows_y, 4, 8, LANES), (columns, LANES)],
        got,
        own,
        wide,
        ay,
    )
    return out


def solution(mesh):
    placed = (P("gx", "gy"), P("gx", None), P("gy", None))
    return jax.shard_map(body, mesh=mesh, in_specs=placed, out_specs=P("gx", "gy"), check_vma=False)
```

```python
import functools

import jax
import jax.numpy as jnp
from jax import lax
from jax.experimental import pallas as pl
from jax.experimental.pallas import tpu as pltpu
from jax.sharding import PartitionSpec as P

F32 = jnp.float32
LANES = 128
VMEM, HBM = (pltpu.MemorySpace.VMEM, pltpu.MemorySpace.HBM)


def iota(shape, dim):
    return lax.broadcasted_iota(jnp.int32, shape, dim)


def take_lanes(values, lanes):
    return jnp.take_along_axis(values, jnp.broadcast_to(lanes, values.shape), axis=1)


def cascade(states, value, decay, gain):
    moved = []
    for state in states:
        value = decay * state + gain * value
        moved.append(value)
    return moved


def toeplitz(column, states):
    return [
        sum((column[row - k] * states[k] for k in range(1, row + 1)), column[row] * states[0])
        for row in range(4)
    ]


def sweep(steps, states, load, decay, gain, store, reverse):
    for step in reversed(range(steps)) if reverse else range(steps):
        states = cascade(states, load(step), decay(step), gain(step))
        if store is not None:
            store(step, states[3])
    return states


def x_ends(
    field_ref, decay_ref, sent_ref, grid_ref, a_ref, near_ref, short_ref, wide_ref, out_ref, sems
):
    levels, steps = decay_ref.shape
    tiles = field_ref.shape[1] // LANES
    copies = [
        pltpu.make_async_copy(decay_ref, short_ref, sems.at[0]),
        pltpu.make_async_copy(field_ref, near_ref, sems.at[1]),
    ]
    for copy in copies:
        copy.start()
    copies[0].wait()
    periodic = jnp.concatenate([short_ref[...]] * (LANES // levels), axis=0).T
    for row in range(4):
        a_ref[:, row, :] = periodic
    grid_ref[:, tiles, :] = jnp.zeros((steps, LANES), F32)
    copies[1].wait()
    for tile in range(tiles):
        grid_ref[:, tile, :] = near_ref[:, tile * LANES : (tile + 1) * LANES]
    row, lane = (iota((4, LANES), 0), iota((4, LANES), 1))
    unit = [((row == tiles) & (lane // levels == k)).astype(F32) for k in range(8)]
    chunk = 16

    def ahead_steps(c, states):
        for step in range(chunk):
            i = c * chunk + step
            a = a_ref[i]
            states = cascade(states, grid_ref[i], a, 1.0 - a)
            out_ref[i] = states[3]
        return tuple(states)

    def back_steps(c, states):
        for step in range(chunk):
            i = steps - 1 - c * chunk - step
            a = a_ref[i]
            states = cascade(states, out_ref[i], a, 1.0 - a)
        return tuple(states)

    ahead = lax.fori_loop(0, steps // chunk, ahead_steps, tuple(unit[:4]))
    back = lax.fori_loop(0, steps // chunk, back_steps, tuple(unit[4:]))
    for k, end in enumerate(ahead + back):
        wide_ref[tiles * k : tiles * (k + 1), :] = end[:tiles]
    first = second = jnp.zeros((4, LANES), F32)
    for k in range(4):
        first += pltpu.roll(jnp.where(lane < 32, back[k], 0.0), 32 * k, 1)
        second += pltpu.roll(jnp.where(lane < 8, ahead[k], 0.0), 16 * k, 1)
        own = jnp.where((lane >= 32) & (lane < 40), back[k], 0.0)
        second += pltpu.roll(own, (16 * k - 24) % LANES, 1)
    wide_ref[24:25, :] = first[tiles:]
    wide_ref[25:26, :] = second[tiles:]
    wide_ref[26:32, :] = jnp.zeros((6, LANES), F32)
    for part in range(sent_ref.shape[1]):
        rows = wide_ref[4 * part : 4 * part + 4, :]
        for device in range(sent_ref.shape[0]):
            sent_ref[device, part] = rows


def y_decays(decay_ref, a_ref):
    decays = decay_ref[...]
    for step in range(decays.shape[1]):
        a_ref[8 * step : 8 * step + 8, :] = lane_of(decays, step)


def lane_of(values, at):
    return jnp.broadcast_to(values[:, at : at + 1], (8, LANES))


def pack(ahead, back, lane):
    half = LANES // 2
    tiles = [jnp.where(lane < half, ahead[k], pltpu.roll(back[k], half, 1)) for k in range(4)]
    packed = jnp.zeros((8, LANES), F32)
    for k in range(4):
        for shift, ends in ((0, back), (8, ahead)):
            at = 16 * k + shift
            moved = pltpu.roll(ends[k], (at - half) % LANES, 1)
            packed = jnp.where((lane >= at) & (lane < at + 8), moved, packed)
    return [*tiles, packed]


def chained(got_ref, head, ahead, back, s_ref, t_ref):
    blocks, half = (got_ref.shape[0], LANES // 2)
    low = iota((8, LANES), 1) < half
    for m in range(blocks):
        at = (m - head) % blocks
        packed = got_ref[at, 4]
        for k in range(4):
            s_ref[m, k] = ahead[k]
        moved = toeplitz([lane_of(packed, 16 * k + 8) for k in range(4)], ahead)
        ahead = [moved[k] + jnp.where(low, got_ref[at, k], 0.0) for k in range(4)]
    for m in reversed(range(blocks)):
        at = (m - head) % blocks
        packed = got_ref[at, 4]
        for k in range(4):
            t_ref[m, k] = back[k]
        moved = toeplitz([lane_of(packed, 16 * k + 4) for k in range(4)], back)
        turned = [
            sum(lane_of(packed, 16 * r + k) * s_ref[m, k] for k in range(4))
            + jnp.where(low, pltpu.roll(got_ref[at, r], half, 1), 0.0)
            for r in range(4)
        ]
        back = [moved[k] + turned[k] for k in range(4)]
    return ahead, back


def x_apply_y_ends(
    got_ref,
    grid_ref,
    ax_ref,
    ay_ref,
    sent_ref,
    wide_ref,
    maps_ref,
    s_ref,
    t_ref,
    z_ref,
    out_ref,
    *,
    head,
):
    steps = grid_ref.shape[0]
    devices, rows = (s_ref.shape[0], 28)
    mine = lax.axis_index("gx")
    first, second = (got_ref[pl.ds(24 + k, devices, stride=rows), :] for k in range(2))
    lane = iota(first.shape, 1) % 8
    for k in range(4):
        for start in range(4):
            maps_ref[4 * k + start] = take_lanes(first, lane + 32 * k + 8 * start)
        maps_ref[16 + k] = take_lanes(second, lane + 16 * k)
        maps_ref[20 + k] = take_lanes(second, lane + 16 * k + 8)

    def end(m, k):
        start = rows * ((m - head) % devices) + 3 * k
        return got_ref[start : start + 4, :]

    def entry(at, m):
        slot = (m - head) % devices
        return maps_ref[at, slot : slot + 1, :]

    zero = jnp.zeros((4, LANES), F32)
    states = [zero] * 4
    for m in range(devices):
        for k in range(4):
            s_ref[m, k] = states[k]
        if m < devices - 1:
            moved = toeplitz([entry(16 + k, m) for k in range(4)], states)
            states = [moved[k] + end(m, k) for k in range(4)]
    states = [zero] * 4
    for m in reversed(range(devices)):
        for k in range(4):
            t_ref[m, k] = states[k]
        if m > 0:
            moved = toeplitz([entry(20 + k, m) for k in range(4)], states)
            turned = [
                sum(entry(4 * r + k, m) * s_ref[m, k] for k in range(4)) + end(m, 4 + r)
                for r in range(4)
            ]
            states = [moved[k] + turned[k] for k in range(4)]
    load_a = lambda i: ax_ref[i]
    gain = lambda i: 1.0 - ax_ref[i]

    def keep(i, value):
        z_ref[i] = value

    start = [s_ref[mine, k] for k in range(4)]
    sweep(steps, start, lambda i: grid_ref[i], load_a, gain, keep, False)
    start = [t_ref[mine, k] for k in range(4)]
    sweep(steps, start, lambda i: z_ref[i], load_a, gain, keep, True)
    wide_ref[...] = jnp.zeros(wide_ref.shape, F32)
    for tile in range(3):
        wide_ref[tile * LANES : (tile + 1) * LANES, :steps] = z_ref[:, tile, :].T

    lane = iota((8, LANES), 1)
    unit = [(lane == steps + k).astype(F32) for k in range(8)]
    count = ay_ref.shape[0] // 8
    load = lambda ref: lambda i: ref[8 * i : 8 * i + 8, :]
    load_a = load(ay_ref)
    gain = lambda i: 1.0 - load_a(i)

    def keep_y(i, value):
        out_ref[8 * i : 8 * i + 8, :] = value

    ahead = sweep(count, unit[:4], load(wide_ref), load_a, gain, keep_y, False)
    back = sweep(count, unit[4:], load(out_ref), load_a, gain, None, True)
    tiles = pack(ahead, back, lane)
    for device in range(sent_ref.shape[0]):
        for k in range(5):
            sent_ref[device, k] = tiles[k]


def y_join(got_ref, sent_ref, mine_ref, s_ref, t_ref, *, head):
    blocks = got_ref.shape[0]
    lane = iota((8, LANES), 1)
    unit = [(lane == LANES // 2 + k).astype(F32) for k in range(8)]
    ahead, back = chained(got_ref, head, unit[:4], unit[4:], s_ref, t_ref)
    tiles = pack(ahead, back, lane)
    for device in range(sent_ref.shape[0]):
        for k in range(5):
            sent_ref[device, k] = tiles[k]
    mine = lax.axis_index("gy") % blocks
    for k in range(4):
        mine_ref[k] = s_ref[mine, k]
        mine_ref[4 + k] = t_ref[mine, k]


def y_apply(
    got_ref,
    mine_ref,
    wide_ref,
    ay_ref,
    field_ref,
    s_ref,
    t_ref,
    z_ref,
    done_ref,
    sems,
    *,
    blocks,
    head,
):
    half = LANES // 2
    zero = [jnp.zeros((8, LANES), F32)] * 4
    chained(got_ref, head, zero, zero, s_ref, t_ref)
    mine = lax.axis_index("gy") // blocks
    ahead = [s_ref[mine, k] for k in range(4)]
    back = [t_ref[mine, k] for k in range(4)]

    def entered(k, starts):
        found = mine_ref[k]
        return found + sum(lane_of(found, half + at) * state for at, state in starts)

    first = [(k, ahead[k]) for k in range(4)]
    both = first + [(4 + k, back[k]) for k in range(4)]
    ahead = [entered(k, first[: k + 1]) for k in range(4)]
    back = [entered(4 + k, both[: 5 + k]) for k in range(4)]
    count = ay_ref.shape[0] // 8
    load = lambda ref: lambda i: ref[8 * i : 8 * i + 8, :]
    load_a = load(ay_ref)
    gain = lambda i: 1.0 - load_a(i)

    def keep(i, value):
        z_ref[8 * i : 8 * i + 8, :] = value

    sweep(count, ahead, load(wide_ref), load_a, gain, keep, False)
    copies, part = ([], LANES // 8)
    for tile in reversed(range(3)):
        shifted = lambda get: lambda i: get(tile * part + i)
        put = lambda i, value: keep(tile * part + i, value)
        back = sweep(part, back, shifted(load(z_ref)), shifted(load_a), shifted(gain), put, True)
        done_ref[tile] = z_ref[tile * LANES : (tile + 1) * LANES, :].T[:half]
        to = field_ref.at[:, tile * LANES : (tile + 1) * LANES]
        copies.append(pltpu.make_async_copy(done_ref.at[tile], to, sems.at[tile]))
        copies[-1].start()
    for copy in copies:
        copy.wait()


def call(kernel, outs, scratch, *args, away_in=0, away_out=0, sems=0):
    here, away = (pl.BlockSpec(memory_space=space) for space in (VMEM, HBM))
    scratch = [pltpu.VMEM(shape, F32) for shape in scratch]
    return pl.pallas_call(
        kernel,
        out_shape=[jax.ShapeDtypeStruct(shape, F32) for shape in outs[:away_out]]
        + [VMEM(shape, F32) for shape in outs[away_out:]],
        in_specs=[away] * away_in + [here] * (len(args) - away_in),
        out_specs=[away] * away_out + [here] * (len(outs) - away_out),
        scratch_shapes=scratch + [pltpu.SemaphoreType.DMA((sems,))] * (sems > 0),
        compiler_params=pltpu.CompilerParams(vmem_limit_bytes=16 << 20),
    )(*(pltpu.with_memory_space_constraint(a, HBM if k < away_in else VMEM) for k, a in enumerate(args)))


def exchange(sent, axis, groups, head):
    groups = [group[head:] + group[:head] for group in groups]
    return lax.all_to_all(sent, axis, 0, 0, tiled=True, axis_index_groups=groups)


def body(field, decay_x, decay_y):
    along_x, along_y = (lax.axis_size("gx"), lax.axis_size("gy"))
    blocks = 8
    rows_y = along_y // blocks
    head_x, head_near, head_far = (along_x * 3 // 4, blocks // 2, rows_y // 2)
    rows, columns = field.shape
    sent, grid, ax = call(
        x_ends,
        [(along_x, 7, 4, LANES), (rows, 4, LANES), (rows, 4, LANES)],
        [(rows, columns), decay_x.T.shape, (32, LANES), (rows, 4, LANES)],
        field,
        decay_x.T,
        away_in=2,
        sems=2,
    )
    got = exchange(sent, "gx", [list(range(along_x))], head_x)
    (ay,) = call(y_decays, [(columns, LANES)], [], decay_y.T)
    sent, wide = call(
        functools.partial(x_apply_y_ends, head=head_x),
        [(blocks, 5, 8, LANES), (columns, LANES)],
        [
            (24, along_x, LANES),
            (along_x, 4, 4, LANES),
            (along_x, 4, 4, LANES),
            (rows, 4, LANES),
            (columns, LANES),
        ],
        got.reshape(along_x * 28, LANES),
        grid,
        ax,
        ay,
    )
    near = [[blocks * r + k for k in range(blocks)] for r in range(rows_y)]
    got = exchange(sent, "gy", near, head_near)
    sent, own = call(
        functools.partial(y_join, head=head_near),
        [(rows_y, 5, 8, LANES), (8, 8, LANES)],
        [(blocks, 4, 8, LANES), (blocks, 4, 8, LANES)],
        got,
    )
    far = [[blocks * r + k for r in range(rows_y)] for k in range(blocks)]
    got = exchange(sent, "gy", far, head_far)
    (out,) = call(
        functools.partial(y_apply, blocks=blocks, head=head_far),
        [(rows, columns)],
        [(rows_y, 4, 8, LANES), (rows_y, 4, 8, LANES), (columns, LANES), (3, rows, LANES)],
        got,
        own,
        wide,
        ay,
        away_out=1,
        sems=3,
    )
    return out


def solution(mesh):
    placed = (P("gx", "gy"), P("gx", None), P("gy", None))
    return jax.shard_map(body, mesh=mesh, in_specs=placed, out_specs=P("gx", "gy"), check_vma=False)
```

```python
import functools

import jax
import jax.numpy as jnp
from jax import lax
from jax.experimental import pallas as pl
from jax.experimental.pallas import tpu as pltpu
from jax.sharding import PartitionSpec as P

F32 = jnp.float32
LANES = 128
VMEM, HBM = (pltpu.MemorySpace.VMEM, pltpu.MemorySpace.HBM)


def iota(shape, dim):
    return lax.broadcasted_iota(jnp.int32, shape, dim)


def take_lanes(values, lanes):
    return jnp.take_along_axis(values, jnp.broadcast_to(lanes, values.shape), axis=1)


def cascade(states, value, decay, gain):
    moved = []
    for state in states:
        value = decay * state + gain * value
        moved.append(value)
    return moved


def toeplitz(column, states):
    return [
        sum((column[row - k] * states[k] for k in range(1, row + 1)), column[row] * states[0])
        for row in range(4)
    ]


def sweep(steps, states, load, decay, gain, store, reverse):
    for step in reversed(range(steps)) if reverse else range(steps):
        states = cascade(states, load(step), decay(step), gain(step))
        if store is not None:
            store(step, states[3])
    return states


def x_ends(
    field_ref,
    decay_ref,
    other_ref,
    sent_ref,
    grid_ref,
    a_ref,
    ay_ref,
    near_ref,
    short_ref,
    turned_ref,
    wide_ref,
    out_ref,
    sems,
):
    levels, steps = decay_ref.shape
    tiles = field_ref.shape[1] // LANES
    copies = [
        pltpu.make_async_copy(decay_ref, short_ref, sems.at[0]),
        pltpu.make_async_copy(other_ref, turned_ref, sems.at[1]),
        pltpu.make_async_copy(field_ref, near_ref, sems.at[2]),
    ]
    for copy in copies:
        copy.start()
    copies[0].wait()
    periodic = jnp.concatenate([short_ref[...]] * (LANES // levels), axis=0).T
    for row in range(4):
        a_ref[:, row, :] = periodic
    grid_ref[:, tiles, :] = jnp.zeros((steps, LANES), F32)
    copies[1].wait()
    y_decays(turned_ref, ay_ref)
    copies[2].wait()
    for tile in range(tiles):
        grid_ref[:, tile, :] = near_ref[:, tile * LANES : (tile + 1) * LANES]
    row, lane = (iota((4, LANES), 0), iota((4, LANES), 1))
    unit = [((row == tiles) & (lane // levels == k)).astype(F32) for k in range(8)]
    chunk = 16

    def ahead_steps(c, states):
        for step in range(chunk):
            i = c * chunk + step
            a = a_ref[i]
            states = cascade(states, grid_ref[i], a, 1.0 - a)
            out_ref[i] = states[3]
        return tuple(states)

    def back_steps(c, states):
        for step in range(chunk):
            i = steps - 1 - c * chunk - step
            a = a_ref[i]
            states = cascade(states, out_ref[i], a, 1.0 - a)
        return tuple(states)

    ahead = lax.fori_loop(0, steps // chunk, ahead_steps, tuple(unit[:4]))
    back = lax.fori_loop(0, steps // chunk, back_steps, tuple(unit[4:]))
    for k, end in enumerate(ahead + back):
        wide_ref[tiles * k : tiles * (k + 1), :] = end[:tiles]
    first = second = jnp.zeros((4, LANES), F32)
    for k in range(4):
        first += pltpu.roll(jnp.where(lane < 32, back[k], 0.0), 32 * k, 1)
        second += pltpu.roll(jnp.where(lane < 8, ahead[k], 0.0), 16 * k, 1)
        own = jnp.where((lane >= 32) & (lane < 40), back[k], 0.0)
        second += pltpu.roll(own, (16 * k - 24) % LANES, 1)
    wide_ref[24:25, :] = first[tiles:]
    wide_ref[25:26, :] = second[tiles:]
    wide_ref[26:32, :] = jnp.zeros((6, LANES), F32)
    for part in range(sent_ref.shape[1]):
        rows = wide_ref[4 * part : 4 * part + 4, :]
        for device in range(sent_ref.shape[0]):
            sent_ref[device, part] = rows


def y_decays(decay_ref, a_ref):
    decays = decay_ref[...]
    for step in range(decays.shape[1]):
        a_ref[8 * step : 8 * step + 8, :] = lane_of(decays, step)


def lane_of(values, at):
    return jnp.broadcast_to(values[:, at : at + 1], (8, LANES))


def pack(ahead, back, lane):
    half = LANES // 2
    tiles = [jnp.where(lane < half, ahead[k], pltpu.roll(back[k], half, 1)) for k in range(4)]
    packed = jnp.zeros((8, LANES), F32)
    for k in range(4):
        for shift, ends in ((0, back), (8, ahead)):
            at = 16 * k + shift
            moved = pltpu.roll(ends[k], (at - half) % LANES, 1)
            packed = jnp.where((lane >= at) & (lane < at + 8), moved, packed)
    return [*tiles, packed]


def chained(got_ref, order, ahead, back, s_ref, t_ref):
    blocks, half = (got_ref.shape[0], LANES // 2)
    low = iota((8, LANES), 1) < half
    for m in range(blocks):
        at = order.index(m)
        packed = got_ref[at, 4]
        for k in range(4):
            s_ref[m, k] = ahead[k]
        moved = toeplitz([lane_of(packed, 16 * k + 8) for k in range(4)], ahead)
        ahead = [moved[k] + jnp.where(low, got_ref[at, k], 0.0) for k in range(4)]
    for m in reversed(range(blocks)):
        at = order.index(m)
        packed = got_ref[at, 4]
        for k in range(4):
            t_ref[m, k] = back[k]
        moved = toeplitz([lane_of(packed, 16 * k + 4) for k in range(4)], back)
        turned = [
            sum(lane_of(packed, 16 * r + k) * s_ref[m, k] for k in range(4))
            + jnp.where(low, pltpu.roll(got_ref[at, r], half, 1), 0.0)
            for r in range(4)
        ]
        back = [moved[k] + turned[k] for k in range(4)]
    return ahead, back


def x_apply_y_ends(
    got_ref,
    grid_ref,
    ax_ref,
    ay_ref,
    sent_ref,
    wide_ref,
    maps_ref,
    s_ref,
    t_ref,
    z_ref,
    out_ref,
    *,
    order,
):
    steps = grid_ref.shape[0]
    devices, rows = (s_ref.shape[0], 28)
    mine = lax.axis_index("gx")
    first, second = (got_ref[pl.ds(24 + k, devices, stride=rows), :] for k in range(2))
    lane = iota(first.shape, 1) % 8
    for k in range(4):
        for start in range(4):
            maps_ref[4 * k + start] = take_lanes(first, lane + 32 * k + 8 * start)
        maps_ref[16 + k] = take_lanes(second, lane + 16 * k)
        maps_ref[20 + k] = take_lanes(second, lane + 16 * k + 8)

    def end(m, k):
        start = rows * order.index(m) + 3 * k
        return got_ref[start : start + 4, :]

    def entry(at, m):
        slot = order.index(m)
        return maps_ref[at, slot : slot + 1, :]

    zero = jnp.zeros((4, LANES), F32)
    states = [zero] * 4
    for m in range(devices):
        for k in range(4):
            s_ref[m, k] = states[k]
        if m < devices - 1:
            moved = toeplitz([entry(16 + k, m) for k in range(4)], states)
            states = [moved[k] + end(m, k) for k in range(4)]
    states = [zero] * 4
    for m in reversed(range(devices)):
        for k in range(4):
            t_ref[m, k] = states[k]
        if m > 0:
            moved = toeplitz([entry(20 + k, m) for k in range(4)], states)
            turned = [
                sum(entry(4 * r + k, m) * s_ref[m, k] for k in range(4)) + end(m, 4 + r)
                for r in range(4)
            ]
            states = [moved[k] + turned[k] for k in range(4)]
    load_a = lambda i: ax_ref[i]
    gain = lambda i: 1.0 - ax_ref[i]

    def keep(i, value):
        z_ref[i] = value

    start = [s_ref[mine, k] for k in range(4)]
    sweep(steps, start, lambda i: grid_ref[i], load_a, gain, keep, False)
    start = [t_ref[mine, k] for k in range(4)]
    sweep(steps, start, lambda i: z_ref[i], load_a, gain, keep, True)
    wide_ref[...] = jnp.zeros(wide_ref.shape, F32)
    for tile in range(3):
        wide_ref[tile * LANES : (tile + 1) * LANES, :steps] = z_ref[:, tile, :].T

    lane = iota((8, LANES), 1)
    unit = [(lane == steps + k).astype(F32) for k in range(8)]
    count = ay_ref.shape[0] // 8
    load = lambda ref: lambda i: ref[8 * i : 8 * i + 8, :]
    load_a = load(ay_ref)
    gain = lambda i: 1.0 - load_a(i)

    def keep_y(i, value):
        out_ref[8 * i : 8 * i + 8, :] = value

    ahead = sweep(count, unit[:4], load(wide_ref), load_a, gain, keep_y, False)
    back = sweep(count, unit[4:], load(out_ref), load_a, gain, None, True)
    tiles = pack(ahead, back, lane)
    for device in range(sent_ref.shape[0]):
        for k in range(5):
            sent_ref[device, k] = tiles[k]


def y_join(got_ref, sent_ref, mine_ref, s_ref, t_ref, *, order):
    blocks = got_ref.shape[0]
    lane = iota((8, LANES), 1)
    unit = [(lane == LANES // 2 + k).astype(F32) for k in range(8)]
    ahead, back = chained(got_ref, order, unit[:4], unit[4:], s_ref, t_ref)
    tiles = pack(ahead, back, lane)
    for device in range(sent_ref.shape[0]):
        for k in range(5):
            sent_ref[device, k] = tiles[k]
    mine = lax.axis_index("gy") % blocks
    for k in range(4):
        mine_ref[k] = s_ref[mine, k]
        mine_ref[4 + k] = t_ref[mine, k]


def y_apply(
    got_ref,
    mine_ref,
    wide_ref,
    ay_ref,
    field_ref,
    s_ref,
    t_ref,
    z_ref,
    done_ref,
    sems,
    *,
    blocks,
    order,
):
    half = LANES // 2
    zero = [jnp.zeros((8, LANES), F32)] * 4
    chained(got_ref, order, zero, zero, s_ref, t_ref)
    mine = lax.axis_index("gy") // blocks
    ahead = [s_ref[mine, k] for k in range(4)]
    back = [t_ref[mine, k] for k in range(4)]

    def entered(k, starts):
        found = mine_ref[k]
        return found + sum(lane_of(found, half + at) * state for at, state in starts)

    first = [(k, ahead[k]) for k in range(4)]
    both = first + [(4 + k, back[k]) for k in range(4)]
    ahead = [entered(k, first[: k + 1]) for k in range(4)]
    back = [entered(4 + k, both[: 5 + k]) for k in range(4)]
    count = ay_ref.shape[0] // 8
    load = lambda ref: lambda i: ref[8 * i : 8 * i + 8, :]
    load_a = load(ay_ref)
    gain = lambda i: 1.0 - load_a(i)

    def keep(i, value):
        z_ref[8 * i : 8 * i + 8, :] = value

    sweep(count, ahead, load(wide_ref), load_a, gain, keep, False)
    copies, part = ([], LANES // 8)
    for tile in reversed(range(3)):
        shifted = lambda get: lambda i: get(tile * part + i)
        put = lambda i, value: keep(tile * part + i, value)
        back = sweep(part, back, shifted(load(z_ref)), shifted(load_a), shifted(gain), put, True)
        done_ref[tile] = z_ref[tile * LANES : (tile + 1) * LANES, :].T[:half]
        to = field_ref.at[:, tile * LANES : (tile + 1) * LANES]
        copies.append(pltpu.make_async_copy(done_ref.at[tile], to, sems.at[tile]))
        copies[-1].start()
    for copy in copies:
        copy.wait()


def call(kernel, outs, scratch, *args, away_in=0, away_out=0, sems=0):
    here, away = (pl.BlockSpec(memory_space=space) for space in (VMEM, HBM))
    scratch = [pltpu.VMEM(shape, F32) for shape in scratch]
    return pl.pallas_call(
        kernel,
        out_shape=[jax.ShapeDtypeStruct(shape, F32) for shape in outs[:away_out]]
        + [VMEM(shape, F32) for shape in outs[away_out:]],
        in_specs=[away] * away_in + [here] * (len(args) - away_in),
        out_specs=[away] * away_out + [here] * (len(outs) - away_out),
        scratch_shapes=scratch + [pltpu.SemaphoreType.DMA((sems,))] * (sems > 0),
        compiler_params=pltpu.CompilerParams(vmem_limit_bytes=16 << 20),
    )(*(pltpu.with_memory_space_constraint(a, HBM if k < away_in else VMEM) for k, a in enumerate(args)))


def exchange(sent, axis, groups, order):
    groups = [[group[k] for k in order] for group in groups]
    return lax.all_to_all(sent, axis, 0, 0, tiled=True, axis_index_groups=groups)


def ring(members, head):
    return [(head + k) % members for k in range(members)]


def far_first(chips, head):
    pairs = [(chip, core) for chip in ring(chips, head)[: chips // 2] for core in (1, 0)]
    return [2 * ((chip + far) % chips) + core for chip, core in pairs for far in (0, chips // 2)]


def body(field, decay_x, decay_y):
    along_x, along_y = (lax.axis_size("gx"), lax.axis_size("gy"))
    blocks = 8
    rows_y = along_y // blocks
    order_x = far_first(along_x // 2, along_x * 3 // 8)
    order_near, order_far = (ring(blocks, blocks // 2), ring(rows_y, rows_y // 2))
    rows, columns = field.shape
    sent, grid, ax, ay = call(
        x_ends,
        [(along_x, 7, 4, LANES), (rows, 4, LANES), (rows, 4, LANES), (columns, LANES)],
        [(rows, columns), decay_x.T.shape, decay_y.T.shape, (32, LANES), (rows, 4, LANES)],
        field,
        decay_x.T,
        decay_y.T,
        away_in=3,
        sems=3,
    )
    got = exchange(sent, "gx", [list(range(along_x))], order_x)
    sent, wide = call(
        functools.partial(x_apply_y_ends, order=order_x),
        [(blocks, 5, 8, LANES), (columns, LANES)],
        [
            (24, along_x, LANES),
            (along_x, 4, 4, LANES),
            (along_x, 4, 4, LANES),
            (rows, 4, LANES),
            (columns, LANES),
        ],
        got.reshape(along_x * 28, LANES),
        grid,
        ax,
        ay,
    )
    near = [[blocks * r + k for k in range(blocks)] for r in range(rows_y)]
    got = exchange(sent, "gy", near, order_near)
    sent, own = call(
        functools.partial(y_join, order=order_near),
        [(rows_y, 5, 8, LANES), (8, 8, LANES)],
        [(blocks, 4, 8, LANES), (blocks, 4, 8, LANES)],
        got,
    )
    far = [[blocks * r + k for r in range(rows_y)] for k in range(blocks)]
    got = exchange(sent, "gy", far, order_far)
    (out,) = call(
        functools.partial(y_apply, blocks=blocks, order=order_far),
        [(rows, columns)],
        [(rows_y, 4, 8, LANES), (rows_y, 4, 8, LANES), (columns, LANES), (3, rows, LANES)],
        got,
        own,
        wide,
        ay,
        away_out=1,
        sems=3,
    )
    return out


def solution(mesh):
    placed = (P("gx", "gy"), P("gx", None), P("gy", None))
    return jax.shard_map(body, mesh=mesh, in_specs=placed, out_specs=P("gx", "gy"), check_vma=False)
```

```python
import functools

import jax
import jax.numpy as jnp
from jax import lax
from jax.experimental import pallas as pl
from jax.experimental.pallas import tpu as pltpu
from jax.sharding import PartitionSpec as P

F32 = jnp.float32
LANES = 128
VMEM, HBM = (pltpu.MemorySpace.VMEM, pltpu.MemorySpace.HBM)


def iota(shape, dim):
    return lax.broadcasted_iota(jnp.int32, shape, dim)


def take_lanes(values, lanes):
    return jnp.take_along_axis(values, jnp.broadcast_to(lanes, values.shape), axis=1)


def cascade(states, value, decay, gain):
    moved = []
    for state in states:
        value = decay * state + gain * value
        moved.append(value)
    return moved


def toeplitz(column, states):
    return [
        sum((column[row - k] * states[k] for k in range(1, row + 1)), column[row] * states[0])
        for row in range(4)
    ]


def sweep(steps, states, load, decay, gain, store, reverse):
    for step in reversed(range(steps)) if reverse else range(steps):
        states = cascade(states, load(step), decay(step), gain(step))
        if store is not None:
            store(step, states[3])
    return states


def x_ends(
    field_ref,
    decay_ref,
    other_ref,
    sent_ref,
    grid_ref,
    a_ref,
    ay_ref,
    near_ref,
    short_ref,
    turned_ref,
    wide_ref,
    out_ref,
    sems,
):
    levels, steps = decay_ref.shape
    tiles = field_ref.shape[1] // LANES
    copies = [
        pltpu.make_async_copy(decay_ref, short_ref, sems.at[0]),
        pltpu.make_async_copy(other_ref, turned_ref, sems.at[1]),
        pltpu.make_async_copy(field_ref, near_ref, sems.at[2]),
    ]
    for copy in copies:
        copy.start()
    copies[0].wait()
    periodic = jnp.concatenate([short_ref[...]] * (LANES // levels), axis=0).T
    for row in range(4):
        a_ref[:, row, :] = periodic
    grid_ref[:, tiles, :] = jnp.zeros((steps, LANES), F32)
    copies[1].wait()
    y_decays(turned_ref, ay_ref)
    copies[2].wait()
    for tile in range(tiles):
        grid_ref[:, tile, :] = near_ref[:, tile * LANES : (tile + 1) * LANES]
    row, lane = (iota((4, LANES), 0), iota((4, LANES), 1))
    unit = [((row == tiles) & (lane // levels == k)).astype(F32) for k in range(8)]
    chunk = 16

    def ahead_steps(c, states):
        for step in range(chunk):
            i = c * chunk + step
            a = a_ref[i]
            states = cascade(states, grid_ref[i], a, 1.0 - a)
            out_ref[i] = states[3]
        return tuple(states)

    def back_steps(c, states):
        for step in range(chunk):
            i = steps - 1 - c * chunk - step
            a = a_ref[i]
            states = cascade(states, out_ref[i], a, 1.0 - a)
        return tuple(states)

    ahead = lax.fori_loop(0, steps // chunk, ahead_steps, tuple(unit[:4]))
    back = lax.fori_loop(0, steps // chunk, back_steps, tuple(unit[4:]))
    for k, end in enumerate(ahead + back):
        wide_ref[tiles * k : tiles * (k + 1), :] = end[:tiles]
    first = second = jnp.zeros((4, LANES), F32)
    for k in range(4):
        first += pltpu.roll(jnp.where(lane < 32, back[k], 0.0), 32 * k, 1)
        second += pltpu.roll(jnp.where(lane < 8, ahead[k], 0.0), 16 * k, 1)
        own = jnp.where((lane >= 32) & (lane < 40), back[k], 0.0)
        second += pltpu.roll(own, (16 * k - 24) % LANES, 1)
    wide_ref[24:25, :] = first[tiles:]
    wide_ref[25:26, :] = second[tiles:]
    for part in range(sent_ref.shape[1]):
        rows = wide_ref[2 * part : 2 * part + 2, :]
        for device in range(sent_ref.shape[0]):
            sent_ref[device, part] = rows


def y_decays(decay_ref, a_ref):
    decays = decay_ref[...]
    for step in range(decays.shape[1]):
        a_ref[8 * step : 8 * step + 8, :] = lane_of(decays, step)


def lane_of(values, at):
    return jnp.broadcast_to(values[:, at : at + 1], (8, LANES))


def pack(ahead, back, lane):
    half = LANES // 2
    tiles = [jnp.where(lane < half, ahead[k], pltpu.roll(back[k], half, 1)) for k in range(4)]
    packed = jnp.zeros((8, LANES), F32)
    for k in range(4):
        for shift, ends in ((0, back), (8, ahead)):
            at = 16 * k + shift
            moved = pltpu.roll(ends[k], (at - half) % LANES, 1)
            packed = jnp.where((lane >= at) & (lane < at + 8), moved, packed)
    folded = jnp.where(lane[:4] < half, packed[:4], pltpu.roll(packed, half, 1)[4:])
    return [part for tile in tiles for part in (tile[:4], tile[4:])] + [folded]


def chained(got_ref, order, ahead, back, s_ref, t_ref, open_ref):
    blocks, half = (got_ref.shape[0], LANES // 2)
    low = iota((8, LANES), 1) < half
    for place in range(blocks):
        for k in range(9):
            open_ref[place, 4 * k : 4 * k + 4, :] = got_ref[place, k]
        open_ref[place, 36:40, :] = pltpu.roll(got_ref[place, 8], half, 1)
    for m in range(blocks):
        at = order.index(m)
        packed = open_ref[at, 32:40, :]
        for k in range(4):
            s_ref[m, k] = ahead[k]
        moved = toeplitz([lane_of(packed, 16 * k + 8) for k in range(4)], ahead)
        ahead = [moved[k] + jnp.where(low, open_ref[at, 8 * k : 8 * k + 8, :], 0.0) for k in range(4)]
    for m in reversed(range(blocks)):
        at = order.index(m)
        packed = open_ref[at, 32:40, :]
        for k in range(4):
            t_ref[m, k] = back[k]
        moved = toeplitz([lane_of(packed, 16 * k + 4) for k in range(4)], back)
        turned = [
            sum(lane_of(packed, 16 * r + k) * s_ref[m, k] for k in range(4))
            + jnp.where(low, pltpu.roll(open_ref[at, 8 * r : 8 * r + 8, :], half, 1), 0.0)
            for r in range(4)
        ]
        back = [moved[k] + turned[k] for k in range(4)]
    return ahead, back


def x_apply_y_ends(
    got_ref,
    grid_ref,
    ax_ref,
    ay_ref,
    sent_ref,
    wide_ref,
    maps_ref,
    s_ref,
    t_ref,
    z_ref,
    out_ref,
    *,
    order,
):
    steps = grid_ref.shape[0]
    devices, rows = (s_ref.shape[0], 26)
    mine = lax.axis_index("gx")
    first, second = (got_ref[pl.ds(24 + k, devices, stride=rows), :] for k in range(2))
    lane = iota(first.shape, 1) % 8
    for k in range(4):
        for start in range(4):
            maps_ref[4 * k + start] = take_lanes(first, lane + 32 * k + 8 * start)
        maps_ref[16 + k] = take_lanes(second, lane + 16 * k)
        maps_ref[20 + k] = take_lanes(second, lane + 16 * k + 8)

    def end(m, k):
        start = rows * order.index(m) + 3 * k
        return got_ref[start : start + 4, :]

    def entry(at, m):
        slot = order.index(m)
        return maps_ref[at, slot : slot + 1, :]

    zero = jnp.zeros((4, LANES), F32)
    states = [zero] * 4
    for m in range(devices):
        for k in range(4):
            s_ref[m, k] = states[k]
        if m < devices - 1:
            moved = toeplitz([entry(16 + k, m) for k in range(4)], states)
            states = [moved[k] + end(m, k) for k in range(4)]
    states = [zero] * 4
    for m in reversed(range(devices)):
        for k in range(4):
            t_ref[m, k] = states[k]
        if m > 0:
            moved = toeplitz([entry(20 + k, m) for k in range(4)], states)
            turned = [
                sum(entry(4 * r + k, m) * s_ref[m, k] for k in range(4)) + end(m, 4 + r)
                for r in range(4)
            ]
            states = [moved[k] + turned[k] for k in range(4)]
    load_a = lambda i: ax_ref[i]
    gain = lambda i: 1.0 - ax_ref[i]

    def keep(i, value):
        z_ref[i] = value

    start = [s_ref[mine, k] for k in range(4)]
    sweep(steps, start, lambda i: grid_ref[i], load_a, gain, keep, False)
    start = [t_ref[mine, k] for k in range(4)]
    sweep(steps, start, lambda i: z_ref[i], load_a, gain, keep, True)
    wide_ref[...] = jnp.zeros(wide_ref.shape, F32)
    for tile in range(3):
        wide_ref[tile * LANES : (tile + 1) * LANES, :steps] = z_ref[:, tile, :].T

    lane = iota((8, LANES), 1)
    unit = [(lane == steps + k).astype(F32) for k in range(8)]
    count = ay_ref.shape[0] // 8
    load = lambda ref: lambda i: ref[8 * i : 8 * i + 8, :]
    load_a = load(ay_ref)
    gain = lambda i: 1.0 - load_a(i)

    def keep_y(i, value):
        out_ref[8 * i : 8 * i + 8, :] = value

    ahead = sweep(count, unit[:4], load(wide_ref), load_a, gain, keep_y, False)
    back = sweep(count, unit[4:], load(out_ref), load_a, gain, None, True)
    tiles = pack(ahead, back, lane)
    for device in range(sent_ref.shape[0]):
        for k in range(9):
            sent_ref[device, k] = tiles[k]


def y_join(got_ref, sent_ref, mine_ref, s_ref, t_ref, open_ref, *, order):
    blocks = got_ref.shape[0]
    lane = iota((8, LANES), 1)
    unit = [(lane == LANES // 2 + k).astype(F32) for k in range(8)]
    ahead, back = chained(got_ref, order, unit[:4], unit[4:], s_ref, t_ref, open_ref)
    tiles = pack(ahead, back, lane)
    for device in range(sent_ref.shape[0]):
        for k in range(9):
            sent_ref[device, k] = tiles[k]
    mine = lax.axis_index("gy") % blocks
    for k in range(4):
        mine_ref[k] = s_ref[mine, k]
        mine_ref[4 + k] = t_ref[mine, k]


def y_apply(
    got_ref,
    mine_ref,
    wide_ref,
    ay_ref,
    field_ref,
    s_ref,
    t_ref,
    open_ref,
    z_ref,
    done_ref,
    sems,
    *,
    blocks,
    order,
):
    half = LANES // 2
    zero = [jnp.zeros((8, LANES), F32)] * 4
    chained(got_ref, order, zero, zero, s_ref, t_ref, open_ref)
    mine = lax.axis_index("gy") // blocks
    ahead = [s_ref[mine, k] for k in range(4)]
    back = [t_ref[mine, k] for k in range(4)]

    def entered(k, starts):
        found = mine_ref[k]
        return found + sum(lane_of(found, half + at) * state for at, state in starts)

    first = [(k, ahead[k]) for k in range(4)]
    both = first + [(4 + k, back[k]) for k in range(4)]
    ahead = [entered(k, first[: k + 1]) for k in range(4)]
    back = [entered(4 + k, both[: 5 + k]) for k in range(4)]
    count = ay_ref.shape[0] // 8
    load = lambda ref: lambda i: ref[8 * i : 8 * i + 8, :]
    load_a = load(ay_ref)
    gain = lambda i: 1.0 - load_a(i)

    def keep(i, value):
        z_ref[8 * i : 8 * i + 8, :] = value

    sweep(count, ahead, load(wide_ref), load_a, gain, keep, False)
    copies, part = ([], LANES // 8)
    for tile in reversed(range(3)):
        shifted = lambda get: lambda i: get(tile * part + i)
        put = lambda i, value: keep(tile * part + i, value)
        back = sweep(part, back, shifted(load(z_ref)), shifted(load_a), shifted(gain), put, True)
        done_ref[tile] = z_ref[tile * LANES : (tile + 1) * LANES, :].T[:half]
        to = field_ref.at[:, tile * LANES : (tile + 1) * LANES]
        copies.append(pltpu.make_async_copy(done_ref.at[tile], to, sems.at[tile]))
        copies[-1].start()
    for copy in copies:
        copy.wait()


def call(kernel, outs, scratch, *args, away_in=0, away_out=0, sems=0):
    here, away = (pl.BlockSpec(memory_space=space) for space in (VMEM, HBM))
    scratch = [pltpu.VMEM(shape, F32) for shape in scratch]
    return pl.pallas_call(
        kernel,
        out_shape=[jax.ShapeDtypeStruct(shape, F32) for shape in outs[:away_out]]
        + [VMEM(shape, F32) for shape in outs[away_out:]],
        in_specs=[away] * away_in + [here] * (len(args) - away_in),
        out_specs=[away] * away_out + [here] * (len(outs) - away_out),
        scratch_shapes=scratch + [pltpu.SemaphoreType.DMA((sems,))] * (sems > 0),
        compiler_params=pltpu.CompilerParams(vmem_limit_bytes=16 << 20),
    )(*(pltpu.with_memory_space_constraint(a, HBM if k < away_in else VMEM) for k, a in enumerate(args)))


def exchange(sent, axis, groups, order):
    groups = [[group[k] for k in order] for group in groups]
    return lax.all_to_all(sent, axis, 0, 0, tiled=True, axis_index_groups=groups)


def ring(members, head):
    return [(head + k) % members for k in range(members)]


def far_first(chips, head):
    pairs = [(chip, core) for chip in ring(chips, head)[: chips // 2] for core in (1, 0)]
    return [2 * ((chip + far) % chips) + core for chip, core in pairs for far in (0, chips // 2)]


def body(field, decay_x, decay_y):
    along_x, along_y = (lax.axis_size("gx"), lax.axis_size("gy"))
    blocks = 8
    rows_y = along_y // blocks
    order_x = far_first(along_x // 2, along_x * 3 // 8)
    order_near, order_far = (ring(blocks, blocks // 2), ring(rows_y, rows_y // 2))
    rows, columns = field.shape
    sent, grid, ax, ay = call(
        x_ends,
        [(along_x, 13, 2, LANES), (rows, 4, LANES), (rows, 4, LANES), (columns, LANES)],
        [(rows, columns), decay_x.T.shape, decay_y.T.shape, (32, LANES), (rows, 4, LANES)],
        field,
        decay_x.T,
        decay_y.T,
        away_in=3,
        sems=3,
    )
    got = exchange(sent, "gx", [list(range(along_x))], order_x)
    sent, wide = call(
        functools.partial(x_apply_y_ends, order=order_x),
        [(blocks, 9, 4, LANES), (columns, LANES)],
        [
            (24, along_x, LANES),
            (along_x, 4, 4, LANES),
            (along_x, 4, 4, LANES),
            (rows, 4, LANES),
            (columns, LANES),
        ],
        got.reshape(along_x * 26, LANES),
        grid,
        ax,
        ay,
    )
    near = [[blocks * r + k for k in range(blocks)] for r in range(rows_y)]
    got = exchange(sent, "gy", near, order_near)
    sent, own = call(
        functools.partial(y_join, order=order_near),
        [(rows_y, 9, 4, LANES), (8, 8, LANES)],
        [(blocks, 4, 8, LANES), (blocks, 4, 8, LANES), (blocks, 40, LANES)],
        got,
    )
    far = [[blocks * r + k for r in range(rows_y)] for k in range(blocks)]
    got = exchange(sent, "gy", far, order_far)
    (out,) = call(
        functools.partial(y_apply, blocks=blocks, order=order_far),
        [(rows, columns)],
        [
            (rows_y, 4, 8, LANES),
            (rows_y, 4, 8, LANES),
            (rows_y, 40, LANES),
            (columns, LANES),
            (3, rows, LANES),
        ],
        got,
        own,
        wide,
        ay,
        away_out=1,
        sems=3,
    )
    return out


def solution(mesh):
    placed = (P("gx", "gy"), P("gx", None), P("gy", None))
    return jax.shard_map(body, mesh=mesh, in_specs=placed, out_specs=P("gx", "gy"), check_vma=False)
```

```python
import functools

import jax
import jax.numpy as jnp
from jax import lax
from jax.experimental import pallas as pl
from jax.experimental.pallas import tpu as pltpu
from jax.sharding import PartitionSpec as P

F32 = jnp.float32
LANES = 128
VMEM, HBM = (pltpu.MemorySpace.VMEM, pltpu.MemorySpace.HBM)


def iota(shape, dim):
    return lax.broadcasted_iota(jnp.int32, shape, dim)


def take_lanes(values, lanes):
    return jnp.take_along_axis(values, jnp.broadcast_to(lanes, values.shape), axis=1)


def cascade(states, value, decay, gain):
    moved = []
    for state in states:
        value = decay * state + gain * value
        moved.append(value)
    return moved


def toeplitz(column, states, added):
    moved = []
    for row in range(4):
        total = added[row]
        for k in range(row + 1):
            total = total + column[row - k] * states[k]
        moved.append(total)
    return moved


def sweep(steps, states, load, decay, gain, store, reverse):
    for step in reversed(range(steps)) if reverse else range(steps):
        states = cascade(states, load(step), decay(step), gain(step))
        if store is not None:
            store(step, states[3])
    return states


def x_ends(
    field_ref,
    decay_ref,
    other_ref,
    sent_ref,
    grid_ref,
    a_ref,
    ay_ref,
    near_ref,
    short_ref,
    turned_ref,
    wide_ref,
    out_ref,
    sems,
):
    levels, steps = decay_ref.shape
    tiles = field_ref.shape[1] // LANES
    copies = [
        pltpu.make_async_copy(decay_ref, short_ref, sems.at[0]),
        pltpu.make_async_copy(other_ref, turned_ref, sems.at[1]),
        pltpu.make_async_copy(field_ref, near_ref, sems.at[2]),
    ]
    for copy in copies:
        copy.start()
    copies[0].wait()
    periodic = jnp.concatenate([short_ref[...]] * (LANES // levels), axis=0).T
    for row in range(4):
        a_ref[:, row, :] = periodic
    grid_ref[:, tiles, :] = jnp.zeros((steps, LANES), F32)
    copies[1].wait()
    y_decays(turned_ref, ay_ref)
    copies[2].wait()
    for tile in range(tiles):
        grid_ref[:, tile, :] = near_ref[:, tile * LANES : (tile + 1) * LANES]
    row, lane = (iota((4, LANES), 0), iota((4, LANES), 1))
    unit = [((row == tiles) & (lane // levels == k)).astype(F32) for k in range(8)]
    chunk = 64

    def ahead_steps(c, states):
        for step in range(chunk):
            i = c * chunk + step
            a = a_ref[i]
            states = cascade(states, grid_ref[i], a, 1.0 - a)
            out_ref[i] = states[3]
        return tuple(states)

    def back_steps(c, states):
        for step in range(chunk):
            i = steps - 1 - c * chunk - step
            a = a_ref[i]
            states = cascade(states, out_ref[i], a, 1.0 - a)
        return tuple(states)

    ahead = lax.fori_loop(0, steps // chunk, ahead_steps, tuple(unit[:4]))
    back = lax.fori_loop(0, steps // chunk, back_steps, tuple(unit[4:]))
    for k, end in enumerate(ahead + back):
        wide_ref[tiles * k : tiles * (k + 1), :] = end[:tiles]
    first = second = jnp.zeros((4, LANES), F32)
    for k in range(4):
        first += pltpu.roll(jnp.where(lane < 32, back[k], 0.0), 32 * k, 1)
        second += pltpu.roll(jnp.where(lane < 8, ahead[k], 0.0), 16 * k, 1)
        own = jnp.where((lane >= 32) & (lane < 40), back[k], 0.0)
        second += pltpu.roll(own, (16 * k - 24) % LANES, 1)
    wide_ref[24:25, :] = first[tiles:]
    wide_ref[25:26, :] = second[tiles:]
    for part in range(sent_ref.shape[1]):
        rows = wide_ref[2 * part : 2 * part + 2, :]
        for device in range(sent_ref.shape[0]):
            sent_ref[device, part] = rows


def y_decays(decay_ref, a_ref):
    decays = decay_ref[...]
    for step in range(decays.shape[1]):
        a_ref[8 * step : 8 * step + 8, :] = lane_of(decays, step)


def lane_of(values, at):
    return jnp.broadcast_to(values[:, at : at + 1], (8, LANES))


def pack(ahead, back, lane):
    half = LANES // 2
    tiles = [jnp.where(lane < half, ahead[k], pltpu.roll(back[k], half, 1)) for k in range(4)]
    packed = jnp.zeros((8, LANES), F32)
    for k in range(4):
        for shift, ends in ((0, back), (8, ahead)):
            at = 16 * k + shift
            moved = pltpu.roll(ends[k], (at - half) % LANES, 1)
            packed = jnp.where((lane >= at) & (lane < at + 8), moved, packed)
    folded = jnp.where(lane[:4] < half, packed[:4], pltpu.roll(packed, half, 1)[4:])
    return [part for tile in tiles for part in (tile[:4], tile[4:])] + [folded]


def chained(got_ref, order, ahead, back, s_ref, t_ref, maps_ref):
    blocks, half = (s_ref.shape[0], LANES // 2)
    low = iota((8, LANES), 1) < half

    def tile(m, k):
        start = 36 * order.index(m) + 8 * k
        return got_ref[start : start + 8, :]

    for place in range(blocks):
        folded = got_ref[36 * place + 32 : 36 * place + 36, :]
        maps_ref[place, :4, :] = folded
        maps_ref[place, 4:, :] = pltpu.roll(folded, half, 1)
    for m in range(blocks):
        packed = maps_ref[order.index(m)]
        for k in range(4):
            s_ref[m, k] = ahead[k]
        ends = [jnp.where(low, tile(m, k), 0.0) for k in range(4)]
        ahead = toeplitz([lane_of(packed, 16 * k + 8) for k in range(4)], ahead, ends)
    for m in reversed(range(blocks)):
        packed = maps_ref[order.index(m)]
        for k in range(4):
            t_ref[m, k] = back[k]
        turned = [
            sum(lane_of(packed, 16 * r + k) * s_ref[m, k] for k in range(4))
            + jnp.where(low, pltpu.roll(tile(m, r), half, 1), 0.0)
            for r in range(4)
        ]
        back = toeplitz([lane_of(packed, 16 * k + 4) for k in range(4)], back, turned)
    return ahead, back


def x_apply_y_ends(
    got_ref,
    grid_ref,
    ax_ref,
    ay_ref,
    sent_ref,
    wide_ref,
    maps_ref,
    s_ref,
    t_ref,
    z_ref,
    out_ref,
    *,
    order,
):
    steps = grid_ref.shape[0]
    devices, rows = (s_ref.shape[0], 26)
    mine = lax.axis_index("gx")
    first, second = (got_ref[pl.ds(24 + k, devices, stride=rows), :] for k in range(2))
    lane = iota(first.shape, 1) % 8
    for k in range(4):
        for start in range(4):
            maps_ref[4 * k + start] = take_lanes(first, lane + 32 * k + 8 * start)
        maps_ref[16 + k] = take_lanes(second, lane + 16 * k)
        maps_ref[20 + k] = take_lanes(second, lane + 16 * k + 8)

    def end(m, k):
        start = rows * order.index(m) + 3 * k
        return got_ref[start : start + 4, :]

    def entry(at, m):
        slot = order.index(m)
        return maps_ref[at, slot : slot + 1, :]

    zero = jnp.zeros((4, LANES), F32)
    states = [zero] * 4
    for m in range(devices):
        for k in range(4):
            s_ref[m, k] = states[k]
        if m < devices - 1:
            column = [entry(16 + k, m) for k in range(4)]
            states = toeplitz(column, states, [end(m, k) for k in range(4)])
    states = [zero] * 4
    for m in reversed(range(devices)):
        for k in range(4):
            t_ref[m, k] = states[k]
        if m > 0:
            turned = [
                sum(entry(4 * r + k, m) * s_ref[m, k] for k in range(4)) + end(m, 4 + r)
                for r in range(4)
            ]
            states = toeplitz([entry(20 + k, m) for k in range(4)], states, turned)
    load_a = lambda i: ax_ref[i]
    gain = lambda i: 1.0 - ax_ref[i]

    def keep(i, value):
        z_ref[i] = value

    start = [s_ref[mine, k] for k in range(4)]
    sweep(steps, start, lambda i: grid_ref[i], load_a, gain, keep, False)
    start = [t_ref[mine, k] for k in range(4)]
    sweep(steps, start, lambda i: z_ref[i], load_a, gain, keep, True)
    wide_ref[...] = jnp.zeros(wide_ref.shape, F32)
    for tile in range(3):
        wide_ref[tile * LANES : (tile + 1) * LANES, :steps] = z_ref[:, tile, :].T

    lane = iota((8, LANES), 1)
    unit = [(lane == steps + k).astype(F32) for k in range(8)]
    count = ay_ref.shape[0] // 8
    load = lambda ref: lambda i: ref[8 * i : 8 * i + 8, :]
    load_a = load(ay_ref)
    gain = lambda i: 1.0 - load_a(i)

    def keep_y(i, value):
        out_ref[8 * i : 8 * i + 8, :] = value

    ahead = sweep(count, unit[:4], load(wide_ref), load_a, gain, keep_y, False)
    back = sweep(count, unit[4:], load(out_ref), load_a, gain, None, True)
    tiles = pack(ahead, back, lane)
    for device in range(sent_ref.shape[0]):
        for k in range(9):
            sent_ref[device, k] = tiles[k]


def y_join(got_ref, sent_ref, mine_ref, s_ref, t_ref, maps_ref, *, order):
    blocks = s_ref.shape[0]
    lane = iota((8, LANES), 1)
    unit = [(lane == LANES // 2 + k).astype(F32) for k in range(8)]
    ahead, back = chained(got_ref, order, unit[:4], unit[4:], s_ref, t_ref, maps_ref)
    tiles = pack(ahead, back, lane)
    for device in range(sent_ref.shape[0]):
        for k in range(9):
            sent_ref[device, k] = tiles[k]
    mine = lax.axis_index("gy") % blocks
    for k in range(4):
        mine_ref[k] = s_ref[mine, k]
        mine_ref[4 + k] = t_ref[mine, k]


def y_apply(
    got_ref,
    mine_ref,
    wide_ref,
    ay_ref,
    field_ref,
    s_ref,
    t_ref,
    maps_ref,
    z_ref,
    done_ref,
    sems,
    *,
    blocks,
    order,
):
    half = LANES // 2
    zero = [jnp.zeros((8, LANES), F32)] * 4
    chained(got_ref, order, zero, zero, s_ref, t_ref, maps_ref)
    mine = lax.axis_index("gy") // blocks
    ahead = [s_ref[mine, k] for k in range(4)]
    back = [t_ref[mine, k] for k in range(4)]

    def entered(k, starts):
        found = mine_ref[k]
        return found + sum(lane_of(found, half + at) * state for at, state in starts)

    first = [(k, ahead[k]) for k in range(4)]
    both = first + [(4 + k, back[k]) for k in range(4)]
    ahead = [entered(k, first[: k + 1]) for k in range(4)]
    back = [entered(4 + k, both[: 5 + k]) for k in range(4)]
    count = ay_ref.shape[0] // 8
    load = lambda ref: lambda i: ref[8 * i : 8 * i + 8, :]
    load_a = load(ay_ref)
    gain = lambda i: 1.0 - load_a(i)

    def keep(i, value):
        z_ref[8 * i : 8 * i + 8, :] = value

    sweep(count, ahead, load(wide_ref), load_a, gain, keep, False)
    copies, part = ([], LANES // 8)
    for tile in reversed(range(3)):
        shifted = lambda get: lambda i: get(tile * part + i)
        put = lambda i, value: keep(tile * part + i, value)
        back = sweep(part, back, shifted(load(z_ref)), shifted(load_a), shifted(gain), put, True)
        done_ref[tile] = z_ref[tile * LANES : (tile + 1) * LANES, :].T[:half]
        to = field_ref.at[:, tile * LANES : (tile + 1) * LANES]
        copies.append(pltpu.make_async_copy(done_ref.at[tile], to, sems.at[tile]))
        copies[-1].start()
    for copy in copies:
        copy.wait()


def call(kernel, outs, scratch, *args, away_in=0, away_out=0, sems=0):
    here, away = (pl.BlockSpec(memory_space=space) for space in (VMEM, HBM))
    scratch = [pltpu.VMEM(shape, F32) for shape in scratch]
    return pl.pallas_call(
        kernel,
        out_shape=[jax.ShapeDtypeStruct(shape, F32) for shape in outs[:away_out]]
        + [VMEM(shape, F32) for shape in outs[away_out:]],
        in_specs=[away] * away_in + [here] * (len(args) - away_in),
        out_specs=[away] * away_out + [here] * (len(outs) - away_out),
        scratch_shapes=scratch + [pltpu.SemaphoreType.DMA((sems,))] * (sems > 0),
        compiler_params=pltpu.CompilerParams(vmem_limit_bytes=16 << 20),
    )(*(pltpu.with_memory_space_constraint(a, HBM if k < away_in else VMEM) for k, a in enumerate(args)))


def exchange(sent, axis, groups, order):
    groups = [[group[k] for k in order] for group in groups]
    return lax.all_to_all(sent, axis, 0, 0, tiled=True, axis_index_groups=groups)


def ring(members, head):
    return [(head + k) % members for k in range(members)]


def far_first(chips, head):
    pairs = [(chip, core) for chip in ring(chips, head)[: chips // 2] for core in (1, 0)]
    return [2 * ((chip + far) % chips) + core for chip, core in pairs for far in (0, chips // 2)]


def body(field, decay_x, decay_y):
    along_x, along_y = (lax.axis_size("gx"), lax.axis_size("gy"))
    blocks = 8
    rows_y = along_y // blocks
    order_x = far_first(along_x // 2, along_x * 3 // 8)
    order_near, order_far = (ring(blocks, blocks // 2), ring(rows_y, rows_y // 2))
    rows, columns = field.shape
    sent, grid, ax, ay = call(
        x_ends,
        [(along_x, 13, 2, LANES), (rows, 4, LANES), (rows, 4, LANES), (columns, LANES)],
        [(rows, columns), decay_x.T.shape, decay_y.T.shape, (32, LANES), (rows, 4, LANES)],
        field,
        decay_x.T,
        decay_y.T,
        away_in=3,
        sems=3,
    )
    got = exchange(sent, "gx", [list(range(along_x))], order_x)
    sent, wide = call(
        functools.partial(x_apply_y_ends, order=order_x),
        [(blocks, 9, 4, LANES), (columns, LANES)],
        [
            (24, along_x, LANES),
            (along_x, 4, 4, LANES),
            (along_x, 4, 4, LANES),
            (rows, 4, LANES),
            (columns, LANES),
        ],
        got.reshape(along_x * 26, LANES),
        grid,
        ax,
        ay,
    )
    near = [[blocks * r + k for k in range(blocks)] for r in range(rows_y)]
    got = exchange(sent, "gy", near, order_near)
    sent, own = call(
        functools.partial(y_join, order=order_near),
        [(rows_y, 9, 4, LANES), (8, 8, LANES)],
        [(blocks, 4, 8, LANES), (blocks, 4, 8, LANES), (blocks, 8, LANES)],
        got.reshape(blocks * 36, LANES),
    )
    far = [[blocks * r + k for r in range(rows_y)] for k in range(blocks)]
    got = exchange(sent, "gy", far, order_far)
    (out,) = call(
        functools.partial(y_apply, blocks=blocks, order=order_far),
        [(rows, columns)],
        [
            (rows_y, 4, 8, LANES),
            (rows_y, 4, 8, LANES),
            (rows_y, 8, LANES),
            (columns, LANES),
            (3, rows, LANES),
        ],
        got.reshape(rows_y * 36, LANES),
        own,
        wide,
        ay,
        away_out=1,
        sems=3,
    )
    return out


def solution(mesh):
    placed = (P("gx", "gy"), P("gx", None), P("gy", None))
    return jax.shard_map(body, mesh=mesh, in_specs=placed, out_specs=P("gx", "gy"), check_vma=False)
```

```python
import functools

import jax
import jax.numpy as jnp
from jax import lax
from jax.experimental import pallas as pl
from jax.experimental.pallas import tpu as pltpu
from jax.sharding import PartitionSpec as P

F32 = jnp.float32
LANES = 128
VMEM, HBM = (pltpu.MemorySpace.VMEM, pltpu.MemorySpace.HBM)


def iota(shape, dim):
    return lax.broadcasted_iota(jnp.int32, shape, dim)


def take_lanes(values, lanes):
    return jnp.take_along_axis(values, jnp.broadcast_to(lanes, values.shape), axis=1)


def cascade(states, value, decay, gain):
    moved = []
    for state in states:
        value = decay * state + gain * value
        moved.append(value)
    return moved


def toeplitz(column, states, added):
    moved = []
    for row in range(4):
        total = added[row]
        for k in range(row + 1):
            total = total + column[row - k] * states[k]
        moved.append(total)
    return moved


def sweep(steps, states, load, decay, gain, store, reverse):
    for step in reversed(range(steps)) if reverse else range(steps):
        states = cascade(states, load(step), decay(step), gain(step))
        if store is not None:
            store(step, states[3])
    return states


def x_ends(
    field_ref,
    decay_ref,
    other_ref,
    sent_ref,
    grid_ref,
    a_ref,
    ay_ref,
    near_ref,
    short_ref,
    turned_ref,
    wide_ref,
    out_ref,
    sems,
):
    levels, steps = decay_ref.shape
    tiles, half = (field_ref.shape[1] // LANES, steps // 2)
    copies = [
        pltpu.make_async_copy(decay_ref, short_ref, sems.at[0]),
        pltpu.make_async_copy(other_ref, turned_ref, sems.at[1]),
        *(
            pltpu.make_async_copy(field_ref.at[part], near_ref.at[part], sems.at[2 + k])
            for k, part in enumerate((pl.ds(0, half), pl.ds(half, half)))
        ),
    ]
    for copy in copies:
        copy.start()
    copies[0].wait()
    periodic = jnp.concatenate([short_ref[...]] * (LANES // levels), axis=0).T
    for row in range(4):
        a_ref[:, row, :] = periodic
    grid_ref[:, tiles, :] = jnp.zeros((steps, LANES), F32)
    copies[1].wait()
    y_decays(turned_ref, ay_ref)
    row, lane = (iota((4, LANES), 0), iota((4, LANES), 1))
    unit = [((row == tiles) & (lane // levels == k)).astype(F32) for k in range(8)]
    chunk = steps

    def back_steps(c, states):
        for step in range(chunk):
            i = steps - 1 - c * chunk - step
            a = a_ref[i]
            states = cascade(states, out_ref[i], a, 1.0 - a)
        return tuple(states)

    ahead = tuple(unit[:4])
    for k in range(2):
        copies[2 + k].wait()
        part = slice(k * half, (k + 1) * half)
        for tile in range(tiles):
            grid_ref[part, tile, :] = near_ref[part, tile * LANES : (tile + 1) * LANES]
        for i in range(k * half, (k + 1) * half):
            a = a_ref[i]
            ahead = tuple(cascade(ahead, grid_ref[i], a, 1.0 - a))
            out_ref[i] = ahead[3]
    back = lax.fori_loop(0, steps // chunk, back_steps, tuple(unit[4:]))
    first = second = jnp.zeros((4, LANES), F32)
    for k in range(4):
        first += pltpu.roll(jnp.where(lane < 32, back[k], 0.0), 32 * k, 1)
        second += pltpu.roll(jnp.where(lane < 8, ahead[k], 0.0), 16 * k, 1)
        own = jnp.where((lane >= 32) & (lane < 40), back[k], 0.0)
        second += pltpu.roll(own, (16 * k - 24) % LANES, 1)
    for start in range(0, wide_ref.shape[0], 26):
        for k, end in enumerate(ahead + back):
            wide_ref[start + tiles * k : start + tiles * (k + 1), :] = end[:tiles]
        wide_ref[start + 24 : start + 25, :] = first[tiles:]
        wide_ref[start + 25 : start + 26, :] = second[tiles:]
    for place in range(wide_ref.shape[0] // 8):
        rows = wide_ref[8 * place : 8 * place + 8, :]
        for start in range(8 * place, sent_ref.shape[0], wide_ref.shape[0]):
            sent_ref[start : start + 8, :] = rows


def y_decays(decay_ref, a_ref):
    decays = decay_ref[...]
    for step in range(decays.shape[1]):
        a_ref[8 * step : 8 * step + 8, :] = lane_of(decays, step)


def lane_of(values, at):
    return jnp.broadcast_to(values[:, at : at + 1], (8, LANES))


def pack(ahead, back, lane):
    half = LANES // 2
    tiles = [jnp.where(lane < half, ahead[k], pltpu.roll(back[k], half, 1)) for k in range(4)]
    packed = jnp.zeros((8, LANES), F32)
    for k in range(4):
        for shift, ends in ((0, back), (8, ahead)):
            at = 16 * k + shift
            moved = pltpu.roll(ends[k], (at - half) % LANES, 1)
            packed = jnp.where((lane >= at) & (lane < at + 8), moved, packed)
    folded = jnp.where(lane[:4] < half, packed[:4], pltpu.roll(packed, half, 1)[4:])
    return [part for tile in tiles for part in (tile[:4], tile[4:])] + [folded]


def chained(got_ref, order, ahead, back, s_ref, t_ref, maps_ref):
    blocks, half = (s_ref.shape[0], LANES // 2)
    low = iota((8, LANES), 1) < half

    def tile(m, k):
        start = 36 * order.index(m) + 8 * k
        return got_ref[start : start + 8, :]

    for place in range(blocks):
        folded = got_ref[36 * place + 32 : 36 * place + 36, :]
        maps_ref[place, :4, :] = folded
        maps_ref[place, 4:, :] = pltpu.roll(folded, half, 1)
    for m in range(blocks):
        packed = maps_ref[order.index(m)]
        for k in range(4):
            s_ref[m, k] = ahead[k]
        ends = [jnp.where(low, tile(m, k), 0.0) for k in range(4)]
        ahead = toeplitz([lane_of(packed, 16 * k + 8) for k in range(4)], ahead, ends)
    for m in reversed(range(blocks)):
        packed = maps_ref[order.index(m)]
        for k in range(4):
            t_ref[m, k] = back[k]
        turned = [
            sum(lane_of(packed, 16 * r + k) * s_ref[m, k] for k in range(4))
            + jnp.where(low, pltpu.roll(tile(m, r), half, 1), 0.0)
            for r in range(4)
        ]
        back = toeplitz([lane_of(packed, 16 * k + 4) for k in range(4)], back, turned)
    return ahead, back


def x_apply_y_ends(
    got_ref,
    grid_ref,
    ax_ref,
    ay_ref,
    sent_ref,
    wide_ref,
    maps_ref,
    s_ref,
    t_ref,
    z_ref,
    out_ref,
    *,
    order,
):
    steps = grid_ref.shape[0]
    devices, rows = (s_ref.shape[0], 26)
    mine = lax.axis_index("gx")
    first, second = (got_ref[pl.ds(24 + k, devices, stride=rows), :] for k in range(2))
    lane = iota(first.shape, 1) % 8
    for k in range(4):
        for start in range(4):
            maps_ref[4 * k + start] = take_lanes(first, lane + 32 * k + 8 * start)
        maps_ref[16 + k] = take_lanes(second, lane + 16 * k)
        maps_ref[20 + k] = take_lanes(second, lane + 16 * k + 8)

    def end(m, k):
        start = rows * order.index(m) + 3 * k
        return got_ref[start : start + 4, :]

    def entry(at, m):
        slot = order.index(m)
        return maps_ref[at, slot : slot + 1, :]

    zero = jnp.zeros((4, LANES), F32)
    states = [zero] * 4
    for m in range(devices):
        for k in range(4):
            s_ref[m, k] = states[k]
        if m < devices - 1:
            column = [entry(16 + k, m) for k in range(4)]
            states = toeplitz(column, states, [end(m, k) for k in range(4)])
    states = [zero] * 4
    for m in reversed(range(devices)):
        for k in range(4):
            t_ref[m, k] = states[k]
        if m > 0:
            turned = [
                sum(entry(4 * r + k, m) * s_ref[m, k] for k in range(4)) + end(m, 4 + r)
                for r in range(4)
            ]
            states = toeplitz([entry(20 + k, m) for k in range(4)], states, turned)
    load_a = lambda i: ax_ref[i]
    gain = lambda i: 1.0 - ax_ref[i]

    def keep(i, value):
        z_ref[i] = value

    start = [s_ref[mine, k] for k in range(4)]
    sweep(steps, start, lambda i: grid_ref[i], load_a, gain, keep, False)
    start = [t_ref[mine, k] for k in range(4)]
    sweep(steps, start, lambda i: z_ref[i], load_a, gain, keep, True)
    wide_ref[...] = jnp.zeros(wide_ref.shape, F32)
    for tile in range(3):
        wide_ref[tile * LANES : (tile + 1) * LANES, :steps] = z_ref[:, tile, :].T

    lane = iota((8, LANES), 1)
    unit = [(lane == steps + k).astype(F32) for k in range(8)]
    count = ay_ref.shape[0] // 8
    load = lambda ref: lambda i: ref[8 * i : 8 * i + 8, :]
    load_a = load(ay_ref)
    gain = lambda i: 1.0 - load_a(i)

    def keep_y(i, value):
        out_ref[8 * i : 8 * i + 8, :] = value

    ahead = sweep(count, unit[:4], load(wide_ref), load_a, gain, keep_y, False)
    back = sweep(count, unit[4:], load(out_ref), load_a, gain, None, True)
    tiles = pack(ahead, back, lane)
    for device in range(sent_ref.shape[0]):
        for k in range(9):
            sent_ref[device, k] = tiles[k]


def y_join(got_ref, sent_ref, mine_ref, s_ref, t_ref, maps_ref, *, order):
    blocks = s_ref.shape[0]
    lane = iota((8, LANES), 1)
    unit = [(lane == LANES // 2 + k).astype(F32) for k in range(8)]
    ahead, back = chained(got_ref, order, unit[:4], unit[4:], s_ref, t_ref, maps_ref)
    tiles = pack(ahead, back, lane)
    for device in range(sent_ref.shape[0]):
        for k in range(9):
            sent_ref[device, k] = tiles[k]
    mine = lax.axis_index("gy") % blocks
    for k in range(4):
        mine_ref[k] = s_ref[mine, k]
        mine_ref[4 + k] = t_ref[mine, k]


def y_apply(
    got_ref,
    mine_ref,
    wide_ref,
    ay_ref,
    field_ref,
    s_ref,
    t_ref,
    maps_ref,
    z_ref,
    done_ref,
    sems,
    *,
    blocks,
    order,
):
    half = LANES // 2
    zero = [jnp.zeros((8, LANES), F32)] * 4
    chained(got_ref, order, zero, zero, s_ref, t_ref, maps_ref)
    mine = lax.axis_index("gy") // blocks
    ahead = [s_ref[mine, k] for k in range(4)]
    back = [t_ref[mine, k] for k in range(4)]

    def entered(k, starts):
        found = mine_ref[k]
        return found + sum(lane_of(found, half + at) * state for at, state in starts)

    first = [(k, ahead[k]) for k in range(4)]
    both = first + [(4 + k, back[k]) for k in range(4)]
    ahead = [entered(k, first[: k + 1]) for k in range(4)]
    back = [entered(4 + k, both[: 5 + k]) for k in range(4)]
    count = ay_ref.shape[0] // 8
    load = lambda ref: lambda i: ref[8 * i : 8 * i + 8, :]
    load_a = load(ay_ref)
    gain = lambda i: 1.0 - load_a(i)

    def keep(i, value):
        z_ref[8 * i : 8 * i + 8, :] = value

    sweep(count, ahead, load(wide_ref), load_a, gain, keep, False)
    copies, part = ([], LANES // 8)
    for tile in reversed(range(3)):
        shifted = lambda get: lambda i: get(tile * part + i)
        put = lambda i, value: keep(tile * part + i, value)
        back = sweep(part, back, shifted(load(z_ref)), shifted(load_a), shifted(gain), put, True)
        done_ref[tile] = z_ref[tile * LANES : (tile + 1) * LANES, :].T[:half]
        to = field_ref.at[:, tile * LANES : (tile + 1) * LANES]
        copies.append(pltpu.make_async_copy(done_ref.at[tile], to, sems.at[tile]))
        copies[-1].start()
    for copy in copies:
        copy.wait()


def call(kernel, outs, scratch, *args, away_in=0, away_out=0, sems=0):
    here, away = (pl.BlockSpec(memory_space=space) for space in (VMEM, HBM))
    scratch = [pltpu.VMEM(shape, F32) for shape in scratch]
    return pl.pallas_call(
        kernel,
        out_shape=[jax.ShapeDtypeStruct(shape, F32) for shape in outs[:away_out]]
        + [VMEM(shape, F32) for shape in outs[away_out:]],
        in_specs=[away] * away_in + [here] * (len(args) - away_in),
        out_specs=[away] * away_out + [here] * (len(outs) - away_out),
        scratch_shapes=scratch + [pltpu.SemaphoreType.DMA((sems,))] * (sems > 0),
        compiler_params=pltpu.CompilerParams(vmem_limit_bytes=16 << 20),
    )(*(pltpu.with_memory_space_constraint(a, HBM if k < away_in else VMEM) for k, a in enumerate(args)))


def exchange(sent, axis, groups, order):
    groups = [[group[k] for k in order] for group in groups]
    return lax.all_to_all(sent, axis, 0, 0, tiled=True, axis_index_groups=groups)


def ring(members, head):
    return [(head + k) % members for k in range(members)]


def far_first(chips, head):
    pairs = [(chip, core) for chip in ring(chips, head)[: chips // 2] for core in (1, 0)]
    return [2 * ((chip + far) % chips) + core for chip, core in pairs for far in (0, chips // 2)]


def body(field, decay_x, decay_y):
    along_x, along_y = (lax.axis_size("gx"), lax.axis_size("gy"))
    blocks = 8
    rows_y = along_y // blocks
    order_x = far_first(along_x // 2, along_x * 3 // 8)
    order_near, order_far = (ring(blocks, blocks // 2), ring(rows_y, rows_y // 2))
    rows, columns = field.shape
    sent, grid, ax, ay = call(
        x_ends,
        [(along_x * 26, LANES), (rows, 4, LANES), (rows, 4, LANES), (columns, LANES)],
        [(rows, columns), decay_x.T.shape, decay_y.T.shape, (4 * 26, LANES), (rows, 4, LANES)],
        field,
        decay_x.T,
        decay_y.T,
        away_in=3,
        sems=4,
    )
    sent = sent.reshape(along_x, 13, 2, LANES)
    got = exchange(sent, "gx", [list(range(along_x))], order_x)
    sent, wide = call(
        functools.partial(x_apply_y_ends, order=order_x),
        [(blocks, 9, 4, LANES), (columns, LANES)],
        [
            (24, along_x, LANES),
            (along_x, 4, 4, LANES),
            (along_x, 4, 4, LANES),
            (rows, 4, LANES),
            (columns, LANES),
        ],
        got.reshape(along_x * 26, LANES),
        grid,
        ax,
        ay,
    )
    near = [[blocks * r + k for k in range(blocks)] for r in range(rows_y)]
    got = exchange(sent, "gy", near, order_near)
    sent, own = call(
        functools.partial(y_join, order=order_near),
        [(rows_y, 9, 4, LANES), (8, 8, LANES)],
        [(blocks, 4, 8, LANES), (blocks, 4, 8, LANES), (blocks, 8, LANES)],
        got.reshape(blocks * 36, LANES),
    )
    far = [[blocks * r + k for r in range(rows_y)] for k in range(blocks)]
    got = exchange(sent, "gy", far, order_far)
    (out,) = call(
        functools.partial(y_apply, blocks=blocks, order=order_far),
        [(rows, columns)],
        [
            (rows_y, 4, 8, LANES),
            (rows_y, 4, 8, LANES),
            (rows_y, 8, LANES),
            (columns, LANES),
            (3, rows, LANES),
        ],
        got.reshape(rows_y * 36, LANES),
        own,
        wide,
        ay,
        away_out=1,
        sems=3,
    )
    return out


def solution(mesh):
    placed = (P("gx", "gy"), P("gx", None), P("gy", None))
    return jax.shard_map(body, mesh=mesh, in_specs=placed, out_specs=P("gx", "gy"), check_vma=False)
```

```python
import functools

import jax
import jax.numpy as jnp
from jax import lax
from jax.experimental import pallas as pl
from jax.experimental.pallas import tpu as pltpu
from jax.sharding import PartitionSpec as P

F32 = jnp.float32
LANES = 128
VMEM, HBM = (pltpu.MemorySpace.VMEM, pltpu.MemorySpace.HBM)


def iota(shape, dim):
    return lax.broadcasted_iota(jnp.int32, shape, dim)


def take_lanes(values, lanes):
    return jnp.take_along_axis(values, jnp.broadcast_to(lanes, values.shape), axis=1)


def cascade(states, value, decay, gain):
    moved = []
    for state in states:
        value = decay * state + gain * value
        moved.append(value)
    return moved


def toeplitz(column, states, added):
    moved = []
    for row in range(4):
        total = added[row]
        for k in range(row + 1):
            total = total + column[row - k] * states[k]
        moved.append(total)
    return moved


def sweep(steps, states, load, decay, gain, store, reverse):
    for step in reversed(range(steps)) if reverse else range(steps):
        states = cascade(states, load(step), decay(step), gain(step))
        if store is not None:
            store(step, states[3])
    return states


def x_ends(
    field_ref,
    decay_ref,
    other_ref,
    sent_ref,
    grid_ref,
    a_ref,
    ay_ref,
    near_ref,
    short_ref,
    turned_ref,
    wide_ref,
    out_ref,
    sems,
):
    levels, steps = decay_ref.shape
    tiles = field_ref.shape[1] // LANES
    copies = [
        pltpu.make_async_copy(decay_ref, short_ref, sems.at[0]),
        pltpu.make_async_copy(other_ref, turned_ref, sems.at[1]),
        pltpu.make_async_copy(field_ref, near_ref, sems.at[2]),
    ]
    for copy in copies:
        copy.start()
    copies[0].wait()
    periodic = jnp.concatenate([short_ref[...]] * (LANES // levels), axis=0).T
    for row in range(4):
        a_ref[:, row, :] = periodic
    grid_ref[:, tiles, :] = jnp.zeros((steps, LANES), F32)
    copies[1].wait()
    y_decays(turned_ref, ay_ref)
    copies[2].wait()
    for tile in range(tiles):
        grid_ref[:, tile, :] = near_ref[:, tile * LANES : (tile + 1) * LANES]
    row, lane = (iota((4, LANES), 0), iota((4, LANES), 1))
    unit = [((row == tiles) & (lane // levels == k)).astype(F32) for k in range(8)]
    chunk = 64

    def ahead_steps(c, states):
        for step in range(chunk):
            i = c * chunk + step
            a = a_ref[i]
            states = cascade(states, grid_ref[i], a, 1.0 - a)
            out_ref[i] = states[3]
        return tuple(states)

    def back_steps(c, states):
        for step in range(chunk):
            i = steps - 1 - c * chunk - step
            a = a_ref[i]
            states = cascade(states, out_ref[i], a, 1.0 - a)
        return tuple(states)

    ahead = lax.fori_loop(0, steps // chunk, ahead_steps, tuple(unit[:4]))
    back = lax.fori_loop(0, steps // chunk, back_steps, tuple(unit[4:]))
    for k, end in enumerate(ahead + back):
        wide_ref[tiles * k : tiles * (k + 1), :] = end[:tiles]
    first = second = jnp.zeros((4, LANES), F32)
    for k in range(4):
        first += pltpu.roll(jnp.where(lane < 32, back[k], 0.0), 32 * k, 1)
        second += pltpu.roll(jnp.where(lane < 8, ahead[k], 0.0), 16 * k, 1)
        own = jnp.where((lane >= 32) & (lane < 40), back[k], 0.0)
        second += pltpu.roll(own, (16 * k - 24) % LANES, 1)
    wide_ref[24:25, :] = first[tiles:]
    wide_ref[25:26, :] = second[tiles:]
    for part in range(sent_ref.shape[1]):
        rows = wide_ref[2 * part : 2 * part + 2, :]
        for device in range(sent_ref.shape[0]):
            sent_ref[device, part] = rows


def y_decays(decay_ref, a_ref):
    decays = decay_ref[...]
    for step in range(decays.shape[1]):
        a_ref[8 * step : 8 * step + 8, :] = lane_of(decays, step)


def lane_of(values, at):
    return jnp.broadcast_to(values[:, at : at + 1], (8, LANES))


def pack(ahead, back, lane):
    half = LANES // 2
    tiles = [jnp.where(lane < half, ahead[k], pltpu.roll(back[k], half, 1)) for k in range(4)]
    packed = jnp.zeros((8, LANES), F32)
    for k in range(4):
        for shift, ends in ((0, back), (8, ahead)):
            at = 16 * k + shift
            moved = pltpu.roll(ends[k], (at - half) % LANES, 1)
            packed = jnp.where((lane >= at) & (lane < at + 8), moved, packed)
    folded = jnp.where(lane[:4] < half, packed[:4], pltpu.roll(packed, half, 1)[4:])
    return [part for tile in tiles for part in (tile[:4], tile[4:])] + [folded]


def chained(got_ref, order, ahead, back, s_ref, t_ref, maps_ref):
    blocks, half = (s_ref.shape[0], LANES // 2)
    low = iota((8, LANES), 1) < half

    def tile(m, k):
        start = 36 * order.index(m) + 8 * k
        return got_ref[start : start + 8, :]

    for place in range(blocks):
        folded = got_ref[36 * place + 32 : 36 * place + 36, :]
        maps_ref[place, :4, :] = folded
        maps_ref[place, 4:, :] = pltpu.roll(folded, half, 1)
    for m in range(blocks):
        packed = maps_ref[order.index(m)]
        for k in range(4):
            s_ref[m, k] = ahead[k]
        ends = [jnp.where(low, tile(m, k), 0.0) for k in range(4)]
        ahead = toeplitz([lane_of(packed, 16 * k + 8) for k in range(4)], ahead, ends)
    for m in reversed(range(blocks)):
        packed = maps_ref[order.index(m)]
        for k in range(4):
            t_ref[m, k] = back[k]
        turned = [
            sum(lane_of(packed, 16 * r + k) * s_ref[m, k] for k in range(4))
            + jnp.where(low, pltpu.roll(tile(m, r), half, 1), 0.0)
            for r in range(4)
        ]
        back = toeplitz([lane_of(packed, 16 * k + 4) for k in range(4)], back, turned)
    return ahead, back


def x_apply_y_ends(
    got_ref,
    grid_ref,
    ax_ref,
    ay_ref,
    sent_ref,
    wide_ref,
    maps_ref,
    s_ref,
    t_ref,
    z_ref,
    out_ref,
    *,
    order,
):
    steps = grid_ref.shape[0]
    devices, rows = (s_ref.shape[0], 26)
    mine = lax.axis_index("gx")
    first, second = (got_ref[pl.ds(24 + k, devices, stride=rows), :] for k in range(2))
    lane = iota(first.shape, 1) % 8
    for k in range(4):
        for start in range(4):
            maps_ref[4 * k + start] = take_lanes(first, lane + 32 * k + 8 * start)
        maps_ref[16 + k] = take_lanes(second, lane + 16 * k)
        maps_ref[20 + k] = take_lanes(second, lane + 16 * k + 8)

    def end(m, k):
        start = rows * order.index(m) + 3 * k
        return got_ref[start : start + 4, :]

    def entry(at, m):
        slot = order.index(m)
        return maps_ref[at, slot : slot + 1, :]

    zero = jnp.zeros((4, LANES), F32)
    states = [zero] * 4
    for m in range(devices):
        for k in range(4):
            s_ref[m, k] = states[k]
        if m < devices - 1:
            column = [entry(16 + k, m) for k in range(4)]
            states = toeplitz(column, states, [end(m, k) for k in range(4)])
    states = [zero] * 4
    for m in reversed(range(devices)):
        for k in range(4):
            t_ref[m, k] = states[k]
        if m > 0:
            turned = [
                sum(entry(4 * r + k, m) * s_ref[m, k] for k in range(4)) + end(m, 4 + r)
                for r in range(4)
            ]
            states = toeplitz([entry(20 + k, m) for k in range(4)], states, turned)
    load_a = lambda i: ax_ref[i]
    gain = lambda i: 1.0 - ax_ref[i]

    def keep(i, value):
        z_ref[i] = value

    start = [s_ref[mine, k] for k in range(4)]
    sweep(steps, start, lambda i: grid_ref[i], load_a, gain, keep, False)
    start = [t_ref[mine, k] for k in range(4)]
    sweep(steps, start, lambda i: z_ref[i], load_a, gain, keep, True)
    empty = jnp.zeros((LANES - steps, LANES), F32)
    for tile in range(3):
        padded = jnp.concatenate([z_ref[:, tile, :], empty], axis=0)
        wide_ref[tile * LANES : (tile + 1) * LANES, :] = padded.T

    lane = iota((8, LANES), 1)
    unit = [(lane == steps + k).astype(F32) for k in range(8)]
    count = ay_ref.shape[0] // 8
    load = lambda ref: lambda i: ref[8 * i : 8 * i + 8, :]
    load_a = load(ay_ref)
    gain = lambda i: 1.0 - load_a(i)

    def keep_y(i, value):
        out_ref[8 * i : 8 * i + 8, :] = value

    ahead = sweep(count, unit[:4], load(wide_ref), load_a, gain, keep_y, False)
    back = sweep(count, unit[4:], load(out_ref), load_a, gain, None, True)
    tiles = pack(ahead, back, lane)
    for device in range(sent_ref.shape[0]):
        for k in range(9):
            sent_ref[device, k] = tiles[k]


def y_join(got_ref, sent_ref, mine_ref, s_ref, t_ref, maps_ref, *, order):
    blocks = s_ref.shape[0]
    lane = iota((8, LANES), 1)
    unit = [(lane == LANES // 2 + k).astype(F32) for k in range(8)]
    ahead, back = chained(got_ref, order, unit[:4], unit[4:], s_ref, t_ref, maps_ref)
    tiles = pack(ahead, back, lane)
    for device in range(sent_ref.shape[0]):
        for k in range(9):
            sent_ref[device, k] = tiles[k]
    mine = lax.axis_index("gy") % blocks
    for k in range(4):
        mine_ref[k] = s_ref[mine, k]
        mine_ref[4 + k] = t_ref[mine, k]


def y_apply(
    got_ref,
    mine_ref,
    wide_ref,
    ay_ref,
    field_ref,
    s_ref,
    t_ref,
    maps_ref,
    z_ref,
    done_ref,
    sems,
    *,
    blocks,
    order,
):
    half = LANES // 2
    zero = [jnp.zeros((8, LANES), F32)] * 4
    chained(got_ref, order, zero, zero, s_ref, t_ref, maps_ref)
    mine = lax.axis_index("gy") // blocks
    ahead = [s_ref[mine, k] for k in range(4)]
    back = [t_ref[mine, k] for k in range(4)]

    def entered(k, starts):
        found = mine_ref[k]
        return found + sum(lane_of(found, half + at) * state for at, state in starts)

    first = [(k, ahead[k]) for k in range(4)]
    both = first + [(4 + k, back[k]) for k in range(4)]
    ahead = [entered(k, first[: k + 1]) for k in range(4)]
    back = [entered(4 + k, both[: 5 + k]) for k in range(4)]
    count = ay_ref.shape[0] // 8
    load = lambda ref: lambda i: ref[8 * i : 8 * i + 8, :]
    load_a = load(ay_ref)
    gain = lambda i: 1.0 - load_a(i)

    def keep(i, value):
        z_ref[8 * i : 8 * i + 8, :] = value

    sweep(count, ahead, load(wide_ref), load_a, gain, keep, False)
    copies, part = ([], LANES // 8)
    for tile in reversed(range(3)):
        shifted = lambda get: lambda i: get(tile * part + i)
        put = lambda i, value: keep(tile * part + i, value)
        back = sweep(part, back, shifted(load(z_ref)), shifted(load_a), shifted(gain), put, True)
        done_ref[tile] = z_ref[tile * LANES : (tile + 1) * LANES, :].T[:half]
        to = field_ref.at[:, tile * LANES : (tile + 1) * LANES]
        copies.append(pltpu.make_async_copy(done_ref.at[tile], to, sems.at[tile]))
        copies[-1].start()
    for copy in copies:
        copy.wait()


def call(kernel, outs, scratch, *args, away_in=0, away_out=0, sems=0):
    here, away = (pl.BlockSpec(memory_space=space) for space in (VMEM, HBM))
    scratch = [pltpu.VMEM(shape, F32) for shape in scratch]
    return pl.pallas_call(
        kernel,
        out_shape=[jax.ShapeDtypeStruct(shape, F32) for shape in outs[:away_out]]
        + [VMEM(shape, F32) for shape in outs[away_out:]],
        in_specs=[away] * away_in + [here] * (len(args) - away_in),
        out_specs=[away] * away_out + [here] * (len(outs) - away_out),
        scratch_shapes=scratch + [pltpu.SemaphoreType.DMA((sems,))] * (sems > 0),
        compiler_params=pltpu.CompilerParams(vmem_limit_bytes=16 << 20),
    )(*(pltpu.with_memory_space_constraint(a, HBM if k < away_in else VMEM) for k, a in enumerate(args)))


def exchange(sent, axis, groups, order):
    groups = [[group[k] for k in order] for group in groups]
    return lax.all_to_all(sent, axis, 0, 0, tiled=True, axis_index_groups=groups)


def ring(members, head):
    return [(head + k) % members for k in range(members)]


def far_first(chips, head):
    pairs = [(chip, core) for chip in ring(chips, head)[: chips // 2] for core in (1, 0)]
    return [2 * ((chip + far) % chips) + core for chip, core in pairs for far in (0, chips // 2)]


def body(field, decay_x, decay_y):
    along_x, along_y = (lax.axis_size("gx"), lax.axis_size("gy"))
    blocks = 8
    rows_y = along_y // blocks
    order_x = far_first(along_x // 2, along_x * 3 // 8)
    order_near, order_far = (ring(blocks, blocks // 2), ring(rows_y, rows_y // 2))
    rows, columns = field.shape
    sent, grid, ax, ay = call(
        x_ends,
        [(along_x, 13, 2, LANES), (rows, 4, LANES), (rows, 4, LANES), (columns, LANES)],
        [(rows, columns), decay_x.T.shape, decay_y.T.shape, (32, LANES), (rows, 4, LANES)],
        field,
        decay_x.T,
        decay_y.T,
        away_in=3,
        sems=3,
    )
    got = exchange(sent, "gx", [list(range(along_x))], order_x)
    sent, wide = call(
        functools.partial(x_apply_y_ends, order=order_x),
        [(blocks, 9, 4, LANES), (columns, LANES)],
        [
            (24, along_x, LANES),
            (along_x, 4, 4, LANES),
            (along_x, 4, 4, LANES),
            (rows, 4, LANES),
            (columns, LANES),
        ],
        got.reshape(along_x * 26, LANES),
        grid,
        ax,
        ay,
    )
    near = [[blocks * r + k for k in range(blocks)] for r in range(rows_y)]
    got = exchange(sent, "gy", near, order_near)
    sent, own = call(
        functools.partial(y_join, order=order_near),
        [(rows_y, 9, 4, LANES), (8, 8, LANES)],
        [(blocks, 4, 8, LANES), (blocks, 4, 8, LANES), (blocks, 8, LANES)],
        got.reshape(blocks * 36, LANES),
    )
    far = [[blocks * r + k for r in range(rows_y)] for k in range(blocks)]
    got = exchange(sent, "gy", far, order_far)
    (out,) = call(
        functools.partial(y_apply, blocks=blocks, order=order_far),
        [(rows, columns)],
        [
            (rows_y, 4, 8, LANES),
            (rows_y, 4, 8, LANES),
            (rows_y, 8, LANES),
            (columns, LANES),
            (3, rows, LANES),
        ],
        got.reshape(rows_y * 36, LANES),
        own,
        wide,
        ay,
        away_out=1,
        sems=3,
    )
    return out


def solution(mesh):
    placed = (P("gx", "gy"), P("gx", None), P("gy", None))
    return jax.shard_map(body, mesh=mesh, in_specs=placed, out_specs=P("gx", "gy"), check_vma=False)
```
